32 devices in a mesh: dp: 2 (over x), tp: 16 (over y, z, core).
Axes of the slice: x: 2, y: 2, z: 4, core: 2. Of those that a mesh axis runs over, the one named last changes fastest.
Arguments:
- x: bfloat16 [5120, 7168], P(('dp', 'tp')), parts along dimension 0
- dy: bfloat16 [5120, 7168], P(('dp', 'tp')), parts along dimension 0
- pre: bfloat16 [5120, 28672], P('dp', 'tp'), parts along dimension 0
- w_in: bfloat16 [7168, 28672], P(None, 'tp')
- w_down: bfloat16 [28672, 7168], P('tp')
Outputs:
- output 1: bfloat16 [5120, 7168], P(('dp', 'tp')), parts along dimension 0
- output 2: bfloat16 [14336, 28672], P('dp', 'tp'), parts along dimension 0
- output 3: bfloat16 [57344, 7168], P(('dp', 'tp')), parts along dimension 0
There are 2 independent parts. The reference program is written for one: setup_inputs(seed, part) draws one part's arguments, and reference() takes and returns one part's arrays. A program takes and returns all parts, laid end to end along the dimension named above; an argument that names none is the same for every part.
All inputs are finite; a program needn't handle non-finite values.
Results may differ from the reference program's by a relative error of at most 0.012.
Values are sent between devices in bfloat16 or wider.
A program may use at most 2 GiB of HBM per device.

```python
import jax
import jax.numpy as jnp

ROWS = 2560
D = 7168
FF = 28672


def act(pre):
    return jax.nn.gelu(pre)


def setup_inputs(seed: int = 0, part: int = 0) -> dict:
    kx, ky, ka, ki, kd = jax.random.split(jax.random.key(seed), 5)
    kx, ky, ka = (jax.random.fold_in(k, part) for k in (kx, ky, ka))
    drawn = {
        "x": jax.random.normal(kx, (ROWS, D), jnp.float32),
        "dy": jax.random.normal(ky, (ROWS, D), jnp.float32),
        "pre": jax.random.normal(ka, (ROWS, FF), jnp.float32),
        "w_in": jax.random.normal(ki, (D, FF), jnp.float32) * D**-0.5,
        "w_down": jax.random.normal(kd, (FF, D), jnp.float32) * FF**-0.5,
    }
    return {k: v.astype(jnp.bfloat16) for k, v in drawn.items()}


def reference(x, dy, pre, w_in, w_down):
    hidden, back = jax.vjp(act, pre.astype(jnp.float32))
    d_hidden = jnp.dot(dy, w_down.T, preferred_element_type=jnp.float32)
    d_pre = back(d_hidden)[0].astype(jnp.bfloat16)
    dx = jnp.dot(d_pre, w_in.T, preferred_element_type=jnp.float32)
    dw_in = jnp.dot(x.T, d_pre, preferred_element_type=jnp.float32)
    dw_down = jnp.dot(hidden.astype(jnp.bfloat16).T, dy, preferred_element_type=jnp.float32)
    return tuple(g.astype(jnp.bfloat16) for g in (dx, dw_in, dw_down))
```

```python
import functools

import jax
import jax.numpy as jnp
from jax import lax
from jax.experimental import pallas as pl
from jax.experimental.pallas import tpu as pltpu

MESH = pl.DeviceIdType.MESH
BF16, F32 = jnp.bfloat16, jnp.float32
NY, NZ, NC = 2, 4, 2
RING = 3
OWN = 5
WINDOW = 2
LAST = 5
ROOT = 0.7978845608028654
CUBE = 0.044715


def bwd_kernel(
    dims,
    x_ref, dy_ref, pre_ref, win_ref, wdn_ref,
    dx_ref, dwin_ref, dwdn_ref, fx_ref, fdy_ref,
    dpre, hidt, in_r, in_l, in_d, in_y,
    rz, ry, rd, szp, szm, sy, sd, rx, sx, lsem,
    r_r, r_l, r_d, r_y, s_r, s_l, s_d, s_y,
    rxz, sxz, rxy, sxy, rxd, sxd, cred,
):
    rows, d, ff, tn, nch, fn = dims
    nt = d // tn
    ck = d // nch
    total = NY * NZ * NC * rows
    t = lax.axis_index("tp")
    c = t % NC
    z = (t // NC) % NZ
    y = t // (NC * NZ)
    yz = y * NZ + z
    p_zp, p_zm = t + NC, t - NC
    p_y = ((1 - y) * NZ + z) * NC + c
    p_d = yz * NC + (1 - c)
    first, last = z == 0, z == NZ - 1

    def remote(src, dst, ssem, rsem, to):
        return pltpu.make_async_remote_copy(
            src, dst, ssem, rsem, device_id={"tp": to}, device_id_type=MESH
        )

    def signal(sem, to):
        pl.semaphore_signal(sem, inc=1, device_id={"tp": to}, device_id_type=MESH)

    def cols(j, width):
        return pl.ds(pl.multiple_of(j * width, width), width)

    def loop(n, body):
        def step(i, carry):
            body(i)
            return carry

        lax.fori_loop(0, n, step, 0)

    barrier = pltpu.get_barrier_semaphore()
    signal(barrier, p_y)
    signal(barrier, p_d)

    @pl.when(jnp.logical_not(last))
    def _():
        signal(barrier, p_zp)

    @pl.when(jnp.logical_not(first))
    def _():
        signal(barrier, p_zm)

    pl.semaphore_wait(barrier, 4 - jnp.where(first | last, 1, 0))

    def zcopy_p(zb, q, src=None):
        ref = fdy_ref.at[y * NZ + zb, c, :, cols(q, ck)]
        return remote(ref if src is None else src, ref, szp.at[zb, q], rz.at[zb, q], p_zp)

    def zcopy_m(zb, q, src=None):
        ref = fdy_ref.at[y * NZ + zb, c, :, cols(q, ck)]
        return remote(ref if src is None else src, ref, szm.at[zb, q], rz.at[zb, q], p_zm)

    def ycopy(zb, q, src=None):
        ref = fdy_ref.at[y * NZ + zb, c, :, cols(q, ck)]
        return remote(ref if src is None else src, ref, sy.at[zb, q], ry.at[zb, q], p_y)

    def dcopy(b, q, src=None):
        ref = fdy_ref.at[b, c, :, cols(q, ck)]
        return remote(ref if src is None else src, ref, sd.at[b, q], rd.at[b, q], p_d)

    def xcopy(k, to):
        return remote(x_ref, fx_ref.at[yz, c], sx.at[k], rx.at[k], to)

    def phase1(wdn, dyu, preu):
        w_load = pltpu.make_async_copy(wdn_ref, wdn, lsem.at[0])
        own_dy = pltpu.make_async_copy(dy_ref, dyu.at[c], lsem.at[1])
        own_x = pltpu.make_async_copy(x_ref, dyu.at[1 - c], lsem.at[2])
        own_dy.start()
        own_x.start()

        def send_own(q):
            src = dy_ref.at[:, cols(q, ck)]

            @pl.when(jnp.logical_not(last))
            def _():
                zcopy_p(z, q, src).start()

            @pl.when(jnp.logical_not(first))
            def _():
                zcopy_m(z, q, src).start()

            ycopy(z, q, src).start()
            dcopy(yz, q, src).start()

        loop(nch, send_own)

        @pl.when(first)
        def _():
            xcopy(0, p_zp).start()

        @pl.when(last)
        def _():
            xcopy(1, p_zm).start()

        own_dy.wait()
        own_x.wait()
        put_dy = pltpu.make_async_copy(dyu.at[c], fdy_ref.at[yz, c], lsem.at[1])
        put_x = pltpu.make_async_copy(dyu.at[1 - c], fx_ref.at[yz, c], lsem.at[2])
        put_dy.start()
        put_x.start()
        w_load.start()

        hr = preu.shape[1] // 128 * 128

        def hidden(r):
            get = pltpu.make_async_copy(
                pre_ref.at[pl.ds(pl.multiple_of(r * hr, hr), hr)], preu.at[0, pl.ds(0, hr)], lsem.at[3]
            )
            get.start()
            get.wait()

            def part(n):
                p = preu[0, pl.ds(0, hr), cols(n, 128)].astype(F32)
                th = jnp.tanh(ROOT * (p + CUBE * (p * p * p)))
                h = (p * (0.5 * (1.0 + th))).astype(BF16)
                hidt[cols(n, 128), cols(r, hr)] = h.T

            loop(ff // 128, part)

        loop(total // hr, hidden)
        put_dy.wait()
        put_x.wait()
        w_load.wait()

        def m1(u):
            get = pltpu.make_async_copy(fdy_ref.at[u], dyu, lsem.at[1])
            get_pre = pltpu.make_async_copy(
                pre_ref.at[pl.ds(pl.multiple_of(u * (NC * rows), NC * rows), NC * rows)], preu.at[0, pl.ds(0, NC * rows)], lsem.at[3]
            )
            get.start()
            get_pre.start()
            get.wait()
            get_pre.wait()

            def part(n):
                acc = lax.dot_general(
                    dyu[...].reshape(NC * rows, d), wdn[cols(n, fn), :], (((1,), (1,)), ((), ())),
                    preferred_element_type=F32,
                )
                p = preu[0, pl.ds(0, NC * rows), cols(n, fn)].astype(F32)
                pp = p * p
                th = jnp.tanh(ROOT * (p + CUBE * (p * pp)))
                slope = 0.5 * (1.0 + th) + (0.5 * p) * (1.0 - th * th) * (ROOT * (1.0 + 3.0 * CUBE * pp))
                dpre[u, :, :, cols(n, fn)] = (acc * slope).astype(BF16).reshape(NC, rows, fn)

            loop(ff // fn, part)

        def wait_d(b):
            loop(nch, lambda q: dcopy_in(b, q).wait_recv())

        def dcopy_in(b, q):
            ref = fdy_ref.at[b, 1 - c, :, cols(q, ck)]
            return remote(ref, ref, sd.at[b, q], rd.at[b, q], p_d)

        def ycopy_in(zb, q):
            ref = fdy_ref.at[(1 - y) * NZ + zb, c, :, cols(q, ck)]
            return remote(ref, ref, sy.at[zb, q], ry.at[zb, q], p_y)

        def pass_row(zb):
            def piece(q):
                zcopy_p(zb, q).wait_recv()

                @pl.when((zb < z) & (z < NZ - 1))
                def _():
                    zcopy_p(zb, q).start()

                @pl.when((zb > z) & (z > 0))
                def _():
                    zcopy_m(zb, q).start()

                ycopy(zb, q).start()
                dcopy(y * NZ + zb, q).start()

            loop(nch, piece)

        def pass_other(zb):
            def piece(q):
                ycopy_in(zb, q).wait_recv()
                dcopy((1 - y) * NZ + zb, q).start()

            loop(nch, piece)

        def unit(b):
            wait_d(b)
            m1(b)

        o1 = jnp.where(z == 0, 1, z - 1)
        o2 = jnp.where(z == NZ - 1, 1, jnp.where(z == 2, 3, 2))
        o3 = jnp.where(z < 2, 3, 0)
        inner = (z == 1) | (z == 2)
        other = (1 - y) * NZ

        unit(yz)
        pass_row(o1)

        @pl.when(z == 1)
        def _():
            xcopy(0, p_zp).start()

        @pl.when(inner)
        def _():
            pass_row(o2)

        @pl.when(z == 2)
        def _():
            xcopy(1, p_zm).start()

        unit(y * NZ + o1)
        pass_other(z)
        unit(other + z)

        @pl.when(jnp.logical_not(inner))
        def _():
            pass_row(o2)

        unit(y * NZ + o2)
        pass_other(o1)
        pass_row(o3)

        @pl.when(z == 2)
        def _():
            xcopy(0, p_zp).start()

        @pl.when(z == 1)
        def _():
            xcopy(1, p_zm).start()

        unit(other + o1)
        unit(y * NZ + o3)
        pass_other(o2)
        unit(other + o2)
        pass_other(o3)
        unit(other + o3)

        def sent(q):
            def row(zb):
                @pl.when((zb <= z) & (z < NZ - 1))
                def _():
                    zcopy_p(zb, q).wait_send()

                @pl.when((zb >= z) & (z > 0))
                def _():
                    zcopy_m(zb, q).wait_send()

                ycopy(zb, q).wait_send()

            loop(NZ, row)
            loop(NY * NZ, lambda b: dcopy(b, q).wait_send())

        loop(nch, sent)

        @pl.when(jnp.logical_not(last))
        def _():
            xcopy(0, p_zp).wait_send()
            remote(x_ref, fx_ref.at[yz + 1, c], sx.at[1], rx.at[1], p_zm).wait_recv()

        @pl.when(jnp.logical_not(first))
        def _():
            xcopy(1, p_zm).wait_send()
            remote(x_ref, fx_ref.at[yz - 1, c], sx.at[0], rx.at[0], p_zp).wait_recv()

    pl.run_scoped(
        phase1,
        pltpu.VMEM((ff, d), BF16),
        pltpu.VMEM((NC, rows, d), BF16),
        pltpu.VMEM((1, max(NC * rows, 128), ff), BF16),
    )

    def phase2(own, out_r, out_l, out_d, out_y, wt, dyt, xt, xtt, odn, oin, odx, ls):
        far = jnp.maximum(z, NZ - 1 - z)
        steps = nt + LAST

        def inside(j):
            return (j >= 0) & (j < nt)

        def rcopy(slot, k):
            return remote(out_r.at[slot, k], in_r.at[slot, k], s_r.at[slot, k], r_r.at[slot, k], p_zp)

        def lcopy(slot, k):
            return remote(out_l.at[slot, k], in_l.at[slot, k], s_l.at[slot, k], r_l.at[slot, k], p_zm)

        def dsum(slot):
            return remote(out_d.at[slot], in_d.at[slot], s_d.at[slot], r_d.at[slot], p_d)

        def ysum(slot):
            return remote(out_y.at[slot], in_y.at[slot], s_y.at[slot], r_y.at[slot], p_y)

        def add_core(s):
            j = s - 1

            @pl.when(inside(j))
            def _():
                slot, ring = j % RING, j % OWN
                dsum(slot).wait_recv()

                def piece(b):
                    own[ring, b // NZ, b % NZ] += in_d[slot, b].astype(F32)

                loop(NY * NZ, piece)

        def along(s, away, edge, copy, inb, outb):
            behind = z if away == 1 else NZ - 1 - z
            j = s - 1 - behind

            @pl.when(inside(j))
            def _():
                slot, ring = j % RING, j % OWN
                for k in range(1, NZ):
                    zz = z + away * k

                    @pl.when((zz >= 0) & (zz < NZ))
                    def _():
                        @pl.when(j >= RING)
                        def _():
                            copy(slot, k - 1).wait_send()

                        @pl.when(edge)
                        def _():
                            def piece(h):
                                outb[slot, k - 1, h] = own[ring, h, zz].astype(BF16)

                            loop(NY, piece)

                        if k < NZ - 1:

                            @pl.when(jnp.logical_not(edge))
                            def _():
                                copy(slot, k).wait_recv()

                                def piece(h):
                                    outb[slot, k - 1, h] = (own[ring, h, zz] + inb[slot, k, h].astype(F32)).astype(BF16)

                                loop(NY, piece)

                        copy(slot, k - 1).start()

                @pl.when(jnp.logical_not(edge))
                def _():
                    copy(slot, 0).wait_recv()

                    def piece(h):
                        own[ring, h, z] += inb[slot, 0, h].astype(F32)

                    loop(NY, piece)

        def across(s):
            j = s - 1 - far

            @pl.when(inside(j))
            def _():
                slot, ring = j % RING, j % OWN

                @pl.when(j >= RING)
                def _():
                    ysum(slot).wait_send()

                out_y[slot] = own[ring, 1 - y, z].astype(BF16)
                ysum(slot).start()

        def put_dx(j):
            return pltpu.make_async_copy(odx.at[j % 2], dx_ref.at[:, cols(j, tn)], ls.at[5, j % 2])

        def finish(s):
            j = s - 2 - far

            @pl.when(inside(j))
            def _():
                slot, ring = j % RING, j % OWN

                @pl.when(j >= 2)
                def _():
                    put_dx(j - 2).wait()

                ysum(slot).wait_recv()
                odx[j % 2] = (own[ring, y, z] + in_y[slot].astype(F32)).astype(BF16)
                put_dx(j).start()

        def xz(j, away, stage, zb):
            ref = fx_ref.at[y * NZ + zb, c, :, cols(j, tn)]
            k = 0 if away == 1 else 1
            return remote(ref, ref, sxz.at[k, stage, j % RING], rxz.at[k, stage, j % RING], p_zp if away == 1 else p_zm)

        def xy(j, row):
            ref = fx_ref.at[pl.ds(row * NZ, NZ), c, :, cols(j, tn)]
            return remote(ref, ref, sxy.at[j % RING], rxy.at[j % RING], p_y)

        def xd(j, core):
            ref = fx_ref.at[:, core, :, cols(j, tn)]
            return remote(ref, ref, sxd.at[j % RING], rxd.at[j % RING], p_d)

        def send(j, make):
            @pl.when(j >= RING)
            def _():
                make(j - RING).wait_send()

            make(j).start()

        def get_x(j):
            return pltpu.make_async_copy(fx_ref.at[:, :, :, cols(j, tn)], xt.at[j % 2], ls.at[2, j % 2])

        inner = (z == 1) | (z == 2)

        def move_x(s):
            @pl.when(inside(s) & inner)
            def _():
                send(s, lambda j: xz(j, 1, 0, z - 1))
                send(s, lambda j: xz(j, -1, 0, z + 1))

            @pl.when(inside(s - 1))
            def _():
                @pl.when(z >= 2)
                def _():
                    xz(s - 1, 1, 0, z - 2).wait_recv()

                @pl.when(z < 2)
                def _():
                    xz(s - 1, -1, 0, z + 2).wait_recv()

                @pl.when(z == 2)
                def _():
                    send(s - 1, lambda j: xz(j, 1, 1, 0))

                @pl.when(z == 1)
                def _():
                    send(s - 1, lambda j: xz(j, -1, 1, 3))

            @pl.when(inside(s - 2))
            def _():
                @pl.when(z == NZ - 1)
                def _():
                    xz(s - 2, 1, 1, 0).wait_recv()

                @pl.when(z == 0)
                def _():
                    xz(s - 2, -1, 1, NZ - 1).wait_recv()

                send(s - 2, lambda j: xy(j, y))

            @pl.when(inside(s - 3))
            def _():
                xy(s - 3, 1 - y).wait_recv()
                send(s - 3, lambda j: xd(j, c))

            @pl.when(inside(s - 4))
            def _():
                xd(s - 4, 1 - c).wait_recv()
                get_x(s - 4).start()

        def get_w(j):
            return pltpu.make_async_copy(win_ref.at[cols(j, tn)], wt.at[j % 2], ls.at[0, j % 2])

        def get_dy(j):
            return pltpu.make_async_copy(fdy_ref.at[:, :, :, cols(j, tn)], dyt.at[j % 2], ls.at[1, j % 2])

        def put_dn(j):
            return pltpu.make_async_copy(odn.at[j % 2], dwdn_ref.at[:, cols(j, tn)], ls.at[3, j % 2])

        def put_in(j):
            return pltpu.make_async_copy(oin.at[j % 2], dwin_ref.at[cols(j, tn)], ls.at[4, j % 2])

        def term(j):
            slot, ring = j % RING, j % OWN
            get_w(j).wait()

            @pl.when(j + 1 < nt)
            def _():
                get_w(j + 1).start()

            @pl.when(j >= RING)
            def _():
                dsum(slot).wait_send()

            def dot(core, h):
                lhs = dpre[pl.ds(h * NZ, NZ), core].reshape(NZ * rows, ff)
                return lax.dot_general(
                    lhs, wt[j % 2], (((1,), (1,)), ((), ())), preferred_element_type=F32
                ).reshape(NZ, rows, tn)

            def theirs(h):
                out_d[slot, pl.ds(h * NZ, NZ)] = dot(1 - c, h).astype(BF16)

            loop(NY, theirs)
            dsum(slot).start()

            def ours(h):
                own[ring, h] = dot(c, h)

            loop(NY, ours)

        mh = ff // 4 if (ff // 4) % 16 == 0 else ff

        def down(j):
            get_dy(j).wait()

            @pl.when(j + 1 < nt)
            def _():
                get_dy(j + 1).start()

            @pl.when(j >= 2)
            def _():
                put_dn(j - 2).wait()

            def part(m):
                at = pl.ds(pl.multiple_of(m * mh, mh), mh)
                odn[j % 2, at] = jnp.dot(
                    hidt[at, :], dyt[j % 2].reshape(total, tn), preferred_element_type=F32
                ).astype(BF16)

            loop(ff // mh, part)
            put_dn(j).start()

        def inward(j):
            get_x(j).wait()

            @pl.when(j >= 2)
            def _():
                put_in(j - 2).wait()

            xtt[...] = xt[j % 2].reshape(total, tn).T

            def part(n):
                rhs = dpre[:, :, :, cols(n, fn)].reshape(total, fn)
                oin[j % 2, :, cols(n, fn)] = jnp.dot(xtt[...], rhs, preferred_element_type=F32).astype(BF16)

            loop(ff // fn, part)
            put_in(j).start()

        get_w(0).start()
        get_dy(0).start()

        def step(s):
            @pl.when(s >= WINDOW)
            def _():
                pl.semaphore_wait(cred.at[2], 1)
                pl.semaphore_wait(cred.at[3], 1)

                @pl.when(jnp.logical_not(last))
                def _():
                    pl.semaphore_wait(cred.at[0], 1)

                @pl.when(jnp.logical_not(first))
                def _():
                    pl.semaphore_wait(cred.at[1], 1)

            add_core(s)
            along(s, 1, first, rcopy, in_r, out_r)
            along(s, -1, last, lcopy, in_l, out_l)
            finish(s)
            across(s)
            move_x(s)

            @pl.when(s < steps - WINDOW)
            def _():
                signal(cred.at[2], p_y)
                signal(cred.at[3], p_d)

                @pl.when(jnp.logical_not(last))
                def _():
                    signal(cred.at[1], p_zp)

                @pl.when(jnp.logical_not(first))
                def _():
                    signal(cred.at[0], p_zm)

            @pl.when(s < nt)
            def _():
                term(s)
                down(s)

            @pl.when(inside(s - LAST))
            def _():
                inward(s - LAST)

        loop(steps, step)

        for j in range(nt - RING, nt):
            slot = j % RING
            for k in range(NZ - 1):

                @pl.when(z + k + 1 < NZ)
                def _():
                    rcopy(slot, k).wait_send()

                @pl.when(z - k - 1 >= 0)
                def _():
                    lcopy(slot, k).wait_send()

            dsum(slot).wait_send()
            ysum(slot).wait_send()
            xy(j, y).wait_send()
            xd(j, c).wait_send()

            @pl.when(inner)
            def _():
                xz(j, 1, 0, z - 1).wait_send()
                xz(j, -1, 0, z + 1).wait_send()

            @pl.when(z == 2)
            def _():
                xz(j, 1, 1, 0).wait_send()

            @pl.when(z == 1)
            def _():
                xz(j, -1, 1, 3).wait_send()

        for j in range(nt - 2, nt):
            put_dn(j).wait()
            put_in(j).wait()
            put_dx(j).wait()

    pl.run_scoped(
        phase2,
        pltpu.VMEM((OWN, NY, NZ, rows, tn), F32),
        pltpu.VMEM((RING, NZ - 1, NY, rows, tn), BF16),
        pltpu.VMEM((RING, NZ - 1, NY, rows, tn), BF16),
        pltpu.VMEM((RING, NY * NZ, rows, tn), BF16),
        pltpu.VMEM((RING, rows, tn), BF16),
        pltpu.VMEM((2, tn, ff), BF16),
        pltpu.VMEM((2, NY * NZ, NC, rows, tn), BF16),
        pltpu.VMEM((2, NY * NZ, NC, rows, tn), BF16),
        pltpu.VMEM((tn, total), BF16),
        pltpu.VMEM((2, ff, tn), BF16),
        pltpu.VMEM((2, tn, ff), BF16),
        pltpu.VMEM((2, rows, tn), BF16),
        pltpu.SemaphoreType.DMA((6, 2)),
    )


def call(rows, d, ff, tn, nch, fn, x, dy, pre, win, wdn):
    blocks = NY * NZ
    total = blocks * NC * rows
    dma = pltpu.SemaphoreType.DMA
    any_ = pl.BlockSpec(memory_space=pl.ANY)
    return pl.pallas_call(
        functools.partial(bwd_kernel, (rows, d, ff, tn, nch, fn)),
        name="bwd",
        out_shape=[
            jax.ShapeDtypeStruct((rows, d), BF16),
            jax.ShapeDtypeStruct((d, ff), BF16),
            jax.ShapeDtypeStruct((ff, d), BF16),
            jax.ShapeDtypeStruct((blocks, NC, rows, d), BF16),
            jax.ShapeDtypeStruct((blocks, NC, rows, d), BF16),
        ],
        in_specs=[any_] * 5,
        out_specs=[any_] * 5,
        scratch_shapes=[
            pltpu.VMEM((blocks, NC, rows, ff), BF16),
            pltpu.VMEM((ff, total), BF16),
            pltpu.VMEM((RING, NZ - 1, NY, rows, tn), BF16),
            pltpu.VMEM((RING, NZ - 1, NY, rows, tn), BF16),
            pltpu.VMEM((RING, blocks, rows, tn), BF16),
            pltpu.VMEM((RING, rows, tn), BF16),
            dma((NZ, nch)), dma((NZ, nch)), dma((blocks, nch)),
            dma((NZ, nch)), dma((NZ, nch)), dma((NZ, nch)), dma((blocks, nch)),
            dma((2,)), dma((2,)), dma((4,)),
            dma((RING, NZ - 1)), dma((RING, NZ - 1)), dma((RING,)), dma((RING,)),
            dma((RING, NZ - 1)), dma((RING, NZ - 1)), dma((RING,)), dma((RING,)),
            dma((2, 2, RING)), dma((2, 2, RING)), dma((RING,)), dma((RING,)), dma((RING,)), dma((RING,)),
            pltpu.SemaphoreType.REGULAR((4,)),
        ],
        compiler_params=pltpu.CompilerParams(
            collective_id=0, has_side_effects=True, vmem_limit_bytes=67043328
        ),
    )(x, dy, pre, win, wdn)


def solution(mesh):
    spec = jax.sharding.PartitionSpec
    rows_of, cols_of = spec(("dp", "tp"), None), spec("dp", "tp")

    def local(x, dy, pre, win, wdn):
        rows, d = x.shape
        ff = pre.shape[1]
        dx, dwin, dwdn, _, _ = call(rows, d, ff, 256, 4, 256, x, dy, pre, win, wdn)
        return dx, dwin, dwdn

    return jax.shard_map(
        local,
        mesh=mesh,
        in_specs=(rows_of, rows_of, cols_of, spec(None, "tp"), spec("tp", None)),
        out_specs=(rows_of, cols_of, rows_of),
        check_vma=False,
    )
```

```python
import functools

import jax
import jax.numpy as jnp
from jax import lax
from jax.experimental import pallas as pl
from jax.experimental.pallas import tpu as pltpu

MESH = pl.DeviceIdType.MESH
BF16, F32 = jnp.bfloat16, jnp.float32
NY, NZ, NC = 2, 4, 2
RING = 4
OWN = 6
WINDOW = 2
TAIL = 4
LEAD = 5
ROOT = 0.7978845608028654
CUBE = 0.044715


def bwd_kernel(
    dims,
    x_ref, dy_ref, pre_ref, win_ref, wdn_ref,
    dx_ref, dwin_ref, dwdn_ref, fx_ref, fdy_ref,
    dpre, hidt, in_r, in_l, in_d, in_y, in_w, in_e,
    rz, ry, rd, szp, szm, sy, sd, rx, sx, lsem,
    r_r, r_l, r_d, r_y, r_w, r_e, s_r, s_l, s_d, s_y, s_w, s_e,
    rxz, sxz, rxy, sxy, rxd, sxd, cred,
):
    rows, d, ff, tn, nch, fn = dims
    nt = d // tn
    ck = d // nch
    total = NY * NZ * NC * rows
    t = lax.axis_index("tp")
    c = t % NC
    z = (t // NC) % NZ
    y = t // (NC * NZ)
    yz = y * NZ + z
    p_zp, p_zm = t + NC, t - NC
    p_y = ((1 - y) * NZ + z) * NC + c
    p_d = yz * NC + (1 - c)
    first, last = z == 0, z == NZ - 1

    def remote(src, dst, ssem, rsem, to):
        return pltpu.make_async_remote_copy(
            src, dst, ssem, rsem, device_id={"tp": to}, device_id_type=MESH
        )

    def signal(sem, to):
        pl.semaphore_signal(sem, inc=1, device_id={"tp": to}, device_id_type=MESH)

    def cols(j, width):
        return pl.ds(pl.multiple_of(j * width, width), width)

    def loop(n, body):
        def step(i, carry):
            body(i)
            return carry

        lax.fori_loop(0, n, step, 0)

    barrier = pltpu.get_barrier_semaphore()
    signal(barrier, p_y)
    signal(barrier, p_d)

    @pl.when(jnp.logical_not(last))
    def _():
        signal(barrier, p_zp)

    @pl.when(jnp.logical_not(first))
    def _():
        signal(barrier, p_zm)

    pl.semaphore_wait(barrier, 4 - jnp.where(first | last, 1, 0))

    inner = (z == 1) | (z == NZ - 2)
    edge = first | last

    def inside(j):
        return (j >= 0) & (j < nt)

    def xz(j, away, stage, zb, n=1):
        ref = fx_ref.at[pl.ds(y * NZ + zb, n), c, :, cols(j, tn)]
        k = 0 if away == 1 else 1
        return remote(ref, ref, sxz.at[k, stage, j % RING], rxz.at[k, stage, j % RING], p_zp if away == 1 else p_zm)

    def xy(j, row):
        ref = fx_ref.at[pl.ds(row * NZ, NZ), c, :, cols(j, tn)]
        return remote(ref, ref, sxy.at[j % RING], rxy.at[j % RING], p_y)

    def xd(j, core):
        ref = fx_ref.at[:, core, :, cols(j, tn)]
        return remote(ref, ref, sxd.at[j % RING], rxd.at[j % RING], p_d)

    def send(j, make):
        @pl.when(j >= RING)
        def _():
            make(j - RING).wait_send()

        make(j).start()

    def x_out(j, away, wait=False):
        end = 2 if away == 1 else 1

        def do(make):
            if wait:
                make(j).wait_send()
            else:
                send(j, make)

        @pl.when(z == end)
        def _():
            do(lambda i: xz(i, away, 0, 1, 2))

        @pl.when(z == NZ - 1 - end)
        def _():
            do(lambda i: xz(i, away, 0, 0 if away == 1 else NZ - 1))

    def move_x(s):
        @pl.when(inside(s))
        def _():
            x_out(s, 1)
            x_out(s, -1)

        @pl.when(inside(s - 2))
        def _():
            j = s - 2

            @pl.when(last)
            def _():
                xz(j, 1, 0, 1, 2).wait_recv()

            @pl.when(first)
            def _():
                xz(j, -1, 0, 1, 2).wait_recv()

            @pl.when(z == 2)
            def _():
                xz(j, 1, 0, 0).wait_recv()
                send(j, lambda i: xz(i, 1, 1, 0))

            @pl.when(z == 1)
            def _():
                xz(j, -1, 0, NZ - 1).wait_recv()
                send(j, lambda i: xz(i, -1, 1, NZ - 1))

        @pl.when(inside(s - 4))
        def _():
            j = s - 4

            @pl.when(last)
            def _():
                xz(j, 1, 1, 0).wait_recv()

            @pl.when(first)
            def _():
                xz(j, -1, 1, NZ - 1).wait_recv()

            send(j, lambda i: xy(i, y))

        @pl.when(inside(s - 6))
        def _():
            xy(s - 6, 1 - y).wait_recv()
            send(s - 6, lambda i: xd(i, c))

    def step_in():
        pl.semaphore_wait(cred.at[2], 1)
        pl.semaphore_wait(cred.at[3], 1)

        @pl.when(jnp.logical_not(last))
        def _():
            pl.semaphore_wait(cred.at[0], 1)

        @pl.when(jnp.logical_not(first))
        def _():
            pl.semaphore_wait(cred.at[1], 1)

    def step_out():
        signal(cred.at[2], p_y)
        signal(cred.at[3], p_d)

        @pl.when(jnp.logical_not(last))
        def _():
            signal(cred.at[1], p_zp)

        @pl.when(jnp.logical_not(first))
        def _():
            signal(cred.at[0], p_zm)

    def dy_at(b, core, q):
        return fdy_ref.at[b, core, :, cols(q, ck)]

    def zcopy(row, zb, q, away, src=None):
        ref = dy_at(row * NZ + zb, c, q)
        back = row != y
        rsem = rz.at[zb, jnp.where(back, nch, q)]
        if away == 1:
            return remote(ref if src is None else src, ref, szp.at[zb, jnp.where(back, nch, q)], rsem, p_zp)
        return remote(ref if src is None else src, ref, szm.at[zb, jnp.where(back, nch, q)], rsem, p_zm)

    def ycopy(row, zb, q, src=None):
        ref = dy_at(row * NZ + zb, c, q)
        return remote(ref if src is None else src, ref, sy.at[zb, q], ry.at[zb, q], p_y)

    def dcopy(b, core, q, src=None):
        ref = dy_at(b, core, q)
        return remote(ref if src is None else src, ref, sd.at[b, q], rd.at[b, q], p_d)

    def xcopy(k, to, b):
        return remote(x_ref, fx_ref.at[b, c], sx.at[k], rx.at[k], to)

    def phase1(wdn, dyu, preu):
        w_load = pltpu.make_async_copy(wdn_ref, wdn, lsem.at[0])
        own_dy = pltpu.make_async_copy(dy_ref, dyu.at[c], lsem.at[1])
        own_x = pltpu.make_async_copy(x_ref, dyu.at[1 - c], lsem.at[2])
        own_dy.start()
        own_x.start()

        def send_own(q):
            src = dy_ref.at[:, cols(q, ck)]

            @pl.when(jnp.logical_not(last))
            def _():
                zcopy(y, z, q, 1, src).start()

            @pl.when(jnp.logical_not(first))
            def _():
                zcopy(y, z, q, -1, src).start()

            ycopy(y, z, q, src).start()
            dcopy(yz, c, q, src).start()

        loop(nch, send_own)
        own_dy.wait()
        own_x.wait()
        put_dy = pltpu.make_async_copy(dyu.at[c], fdy_ref.at[yz, c], lsem.at[1])
        put_x = pltpu.make_async_copy(dyu.at[1 - c], fx_ref.at[yz, c], lsem.at[2])
        put_dy.start()
        put_x.start()
        w_load.start()

        def pass_z(row, zb, q):
            @pl.when((zb < z) & (z < NZ - 1))
            def _():
                zcopy(row, zb, q, 1).start()

            @pl.when((zb > z) & (z > 0))
            def _():
                zcopy(row, zb, q, -1).start()

        def pass_row(zb, q):
            zcopy(y, zb, q, 1).wait_recv()
            pass_z(y, zb, q)

            @pl.when(q > 0)
            def _():
                ycopy(y, zb, q).start()

            dcopy(y * NZ + zb, c, q).start()

        def pass_back(zb):
            zcopy(1 - y, zb, 0, 1).wait_recv()
            pass_z(1 - y, zb, 0)
            dcopy((1 - y) * NZ + zb, c, 0).start()

        def pass_other(zb):
            def piece(q):
                ycopy(1 - y, zb, q + 1).wait_recv()
                dcopy((1 - y) * NZ + zb, c, q + 1).start()

            loop(nch - 1, piece)

        ycopy(1 - y, z, 0).wait_recv()

        @pl.when(jnp.logical_not(last))
        def _():
            zcopy(1 - y, z, 0, 1).start()

        @pl.when(jnp.logical_not(first))
        def _():
            zcopy(1 - y, z, 0, -1).start()

        dcopy((1 - y) * NZ + z, c, 0).start()

        @pl.when(first)
        def _():
            xcopy(0, p_zp, yz).start()

        @pl.when(last)
        def _():
            xcopy(1, p_zm, yz).start()

        hr = preu.shape[0] // 128 * 128

        def hidden(r):
            get = pltpu.make_async_copy(
                pre_ref.at[pl.ds(pl.multiple_of(r * hr, hr), hr)], preu.at[pl.ds(0, hr)], lsem.at[3]
            )
            get.start()
            get.wait()

            def part(n):
                p = preu[pl.ds(0, hr), cols(n, 128)].astype(F32)
                th = jnp.tanh(ROOT * (p + CUBE * (p * p * p)))
                h = (p * (0.5 * (1.0 + th))).astype(BF16)
                hidt[cols(n, 128), cols(r, hr)] = h.T

            loop(ff // 128, part)

        loop(total // hr, hidden)
        put_dy.wait()
        put_x.wait()
        w_load.wait()

        o1 = jnp.where(z == 0, 1, z - 1)
        o2 = jnp.where(z == NZ - 1, 1, jnp.where(z == 2, 3, 2))
        o3 = jnp.where(z < 2, 3, 0)

        def unit(i):
            @pl.when(i == 1)
            def _():
                pass_back(o1)

                @pl.when(z == 1)
                def _():
                    xcopy(0, p_zp, yz).start()

            @pl.when(i == 2)
            def _():
                @pl.when(inner)
                def _():
                    pass_back(o2)

                @pl.when(z == 2)
                def _():
                    xcopy(1, p_zm, yz).start()

                pass_other(z)

            @pl.when((i == 3) & edge)
            def _():
                pass_back(o2)

            @pl.when(i == 4)
            def _():
                pass_other(o1)

            @pl.when(i == 5)
            def _():
                @pl.when(inner)
                def _():
                    pass_back(o3)

                pass_other(o2)

            @pl.when(i == 6)
            def _():
                @pl.when(inner)
                def _():
                    xcopy(0, p_zp, yz - 1).wait_recv()
                    xcopy(1, p_zm, yz + 1).wait_recv()

                move_x(0)
                step_out()
                move_x(1)
                step_out()

            @pl.when(i == 7)
            def _():
                for v in (2, 3):
                    step_in()
                    move_x(v)
                    step_out()

                @pl.when(edge)
                def _():
                    pass_back(o3)

                pass_other(o3)
                step_in()
                move_x(4)
                step_out()

            row = jnp.where((i == 0) | (i == 1) | (i == 3) | (i == 6), y, 1 - y)
            near = jnp.where((i == 0) | (i == 2), z, o1)
            u = row * NZ + jnp.where(i > 5, o3, jnp.where((i == 3) | (i == 5), o2, near))
            loop(nch, lambda q: dcopy(u, 1 - c, q).wait_recv())
            get = pltpu.make_async_copy(fdy_ref.at[u], dyu, lsem.at[1])
            get_pre = pltpu.make_async_copy(
                pre_ref.at[pl.ds(pl.multiple_of(u * (NC * rows), NC * rows), NC * rows)],
                preu.at[pl.ds(0, NC * rows)], lsem.at[3],
            )
            get.start()
            get_pre.start()
            get.wait()
            get_pre.wait()

            def part(n):
                @pl.when(i == 0)
                def _():
                    pass_row(o1, n)

                @pl.when(((i == 1) & inner) | ((i == 2) & edge))
                def _():
                    pass_row(o2, n)

                @pl.when((i == 4) & inner)
                def _():
                    pass_row(o3, n)

                early = (nch - 1) // 2

                @pl.when((i == 4) & edge & (n > 0) & (n % 2 == 0))
                def _():
                    pass_row(o3, n // 2 - 1)

                @pl.when((i == 5) & edge & (n % 2 == 0))
                def _():
                    pass_row(o3, early + n // 2)

                acc = lax.dot_general(
                    dyu[...].reshape(NC * rows, d), wdn[cols(n, fn), :], (((1,), (1,)), ((), ())),
                    preferred_element_type=F32,
                )
                p = preu[pl.ds(0, NC * rows), cols(n, fn)].astype(F32)
                pp = p * p
                th = jnp.tanh(ROOT * (p + CUBE * (p * pp)))
                slope = 0.5 * (1.0 + th) + (0.5 * p) * (1.0 - th * th) * (ROOT * (1.0 + 3.0 * CUBE * pp))
                dpre[u, :, :, cols(n, fn)] = (acc * slope).astype(BF16).reshape(NC, rows, fn)

            loop(nch, part)

        loop(NY * NZ, unit)

        def sent(q):
            def block(zb):
                @pl.when((zb <= z) & (z < NZ - 1))
                def _():
                    zcopy(y, zb, q, 1).wait_send()

                @pl.when((zb >= z) & (z > 0))
                def _():
                    zcopy(y, zb, q, -1).wait_send()

                @pl.when(q == 0)
                def _():
                    @pl.when((zb <= z) & (z < NZ - 1))
                    def _():
                        zcopy(1 - y, zb, q, 1).wait_send()

                    @pl.when((zb >= z) & (z > 0))
                    def _():
                        zcopy(1 - y, zb, q, -1).wait_send()

                @pl.when((q > 0) | (zb == z))
                def _():
                    ycopy(y, zb, q).wait_send()

            loop(NZ, block)
            loop(NY * NZ, lambda b: dcopy(b, c, q).wait_send())

        loop(nch, sent)

        @pl.when(z < 2)
        def _():
            xcopy(0, p_zp, yz).wait_send()

        @pl.when(z >= 2)
        def _():
            xcopy(1, p_zm, yz).wait_send()

    pl.run_scoped(
        phase1,
        pltpu.VMEM((ff, d), BF16),
        pltpu.VMEM((NC, rows, d), BF16),
        pltpu.VMEM((max(NC * rows, 128), ff), BF16),
    )

    def phase2(own, out_r, out_l, out_d, out_y, out_w, out_e, wt, dyt, xt, odn, oin, odx, ls):
        steps = nt + TAIL

        def rcopy(slot, k):
            return remote(out_r.at[slot, k], in_r.at[slot, k], s_r.at[slot, k], r_r.at[slot, k], p_zp)

        def lcopy(slot, k):
            return remote(out_l.at[slot, k], in_l.at[slot, k], s_l.at[slot, k], r_l.at[slot, k], p_zm)

        def dsum(slot):
            return remote(out_d.at[slot], in_d.at[slot], s_d.at[slot], r_d.at[slot], p_d)

        def ysum(slot):
            return remote(out_y.at[slot], in_y.at[slot], s_y.at[slot], r_y.at[slot], p_y)

        def add_core(s):
            j = s - 1

            @pl.when(inside(j))
            def _():
                slot, ring = j % RING, j % OWN
                dsum(slot).wait_recv()

                def piece(b):
                    own[ring, b // NZ, b % NZ] += in_d[slot, b].astype(F32)

                loop(NY * NZ, piece)

        def along(s, away, start, copy, inb, outb):
            behind = z if away == 1 else NZ - 1 - z
            j = s - 1 - behind

            @pl.when(inside(j))
            def _():
                slot, ring = j % RING, j % OWN
                swaps = j % 2 == 0
                for k in range(NZ - 1, 0, -1):
                    zz = z + away * k
                    here = (zz >= 0) & (zz < NZ)
                    if k == 1:
                        here = here & jnp.logical_not(start & swaps)

                    @pl.when(here)
                    def _():
                        @pl.when(j >= RING)
                        def _():
                            copy(slot, k - 1).wait_send()

                        @pl.when(start)
                        def _():
                            def piece(h):
                                outb[slot, k - 1, h] = own[ring, h, zz].astype(BF16)

                            loop(NY, piece)

                        if k < NZ - 1:

                            @pl.when(jnp.logical_not(start))
                            def _():
                                copy(slot, k).wait_recv()

                                def piece(h):
                                    outb[slot, k - 1, h] = (own[ring, h, zz] + inb[slot, k, h].astype(F32)).astype(BF16)

                                loop(NY, piece)

                        copy(slot, k - 1).start()

        def settle(s, away, copy, inb):
            behind = z if away == 1 else NZ - 1 - z
            j = s - behind - jnp.where(behind == NZ - 1, 1, 2)

            @pl.when(inside(j) & ((behind > 1) | ((behind == 1) & (j % 2 == 1))))
            def _():
                slot, ring = j % RING, j % OWN
                copy(slot, 0).wait_recv()

                def piece(h):
                    own[ring, h, z] += inb[slot, 0, h].astype(F32)

                loop(NY, piece)

        nxt = jnp.where(first, 1, NZ - 2)
        p_nxt = jnp.where(first, p_zp, p_zm)
        p_end = jnp.where(z == 1, p_zm, p_zp)

        def wcopy(slot):
            return remote(out_w.at[slot], in_w.at[slot], s_w.at[slot], r_w.at[slot], p_y)

        def ecopy(slot, to):
            return remote(out_e.at[slot], in_e.at[slot], s_e.at[slot], r_e.at[slot], to)

        def swap(s):
            def at(j, where, body):
                @pl.when(inside(j) & (j % 2 == 0) & where)
                def _():
                    body(j % RING, j % OWN, j >= RING)

            def give(slot, ring, again):
                @pl.when(again)
                def _():
                    wcopy(slot).wait_send()

                out_w[slot] = own[ring, 1 - y, nxt].astype(BF16)
                wcopy(slot).start()

            def join(slot, ring, again):
                @pl.when(again)
                def _():
                    ecopy(slot, p_nxt).wait_send()

                wcopy(slot).wait_recv()
                out_e[slot] = (own[ring, y, nxt] + in_w[slot].astype(F32)).astype(BF16)
                ecopy(slot, p_nxt).start()

            def take(slot, ring, again):
                ecopy(slot, p_end).wait_recv()
                own[ring, y, z] += in_e[slot].astype(F32)

            at(s - 1, edge, give)
            at(s - 3, edge, join)
            at(s - 4, inner, take)

        def across(s):
            j = s - 4

            @pl.when(inside(j))
            def _():
                slot, ring = j % RING, j % OWN

                @pl.when(j >= RING)
                def _():
                    ysum(slot).wait_send()

                out_y[slot] = own[ring, 1 - y, z].astype(BF16)
                ysum(slot).start()

        def put_dx(j):
            return pltpu.make_async_copy(odx.at[j % 2], dx_ref.at[:, cols(j, tn)], ls.at[5, j % 2])

        def finish(s):
            j = s - 6

            @pl.when(inside(j))
            def _():
                slot, ring = j % RING, j % OWN

                @pl.when(j >= 2)
                def _():
                    put_dx(j - 2).wait()

                ysum(slot).wait_recv()
                odx[j % 2] = (own[ring, y, z] + in_y[slot].astype(F32)).astype(BF16)
                put_dx(j).start()

        def get_x(j):
            return pltpu.make_async_copy(fx_ref.at[:, :, :, cols(j, tn)], xt.at[j % 2], ls.at[2, j % 2])

        def get_w(j):
            return pltpu.make_async_copy(win_ref.at[cols(j, tn)], wt.at[j % 2], ls.at[0, j % 2])

        def get_dy(j):
            return pltpu.make_async_copy(fdy_ref.at[:, :, :, cols(j, tn)], dyt.at[j % 2], ls.at[1, j % 2])

        def put_dn(j):
            return pltpu.make_async_copy(odn.at[j % 2], dwdn_ref.at[:, cols(j, tn)], ls.at[3, j % 2])

        def put_in(j):
            return pltpu.make_async_copy(oin.at[j % 2], dwin_ref.at[cols(j, tn)], ls.at[4, j % 2])

        def term(j):
            slot, ring = j % RING, j % OWN
            get_w(j).wait()

            @pl.when(j + 1 < nt)
            def _():
                get_w(j + 1).start()

            @pl.when(j >= RING)
            def _():
                dsum(slot).wait_send()

            def dot(core, h):
                lhs = dpre[h * NZ : (h + 1) * NZ, core].reshape(NZ * rows, ff)
                return lax.dot_general(
                    lhs, wt[j % 2], (((1,), (1,)), ((), ())), preferred_element_type=F32
                ).reshape(NZ, rows, tn)

            for h in range(NY):
                out_d[slot, h * NZ : (h + 1) * NZ] = dot(1 - c, h).astype(BF16)
            dsum(slot).start()
            for h in range(NY):
                own[ring, h] = dot(c, h)

        def down(j):
            get_dy(j).wait()

            @pl.when(j + 1 < nt)
            def _():
                get_dy(j + 1).start()

            @pl.when(j >= 2)
            def _():
                put_dn(j - 2).wait()

            rhs = dyt[j % 2].reshape(total, tn)
            for m in range(0, ff, ff // 4):
                odn[j % 2, m : m + ff // 4] = jnp.dot(
                    hidt[m : m + ff // 4], rhs, preferred_element_type=F32
                ).astype(BF16)
            put_dn(j).start()

        def inward(j):
            get_x(j).wait()

            @pl.when(j >= 2)
            def _():
                put_in(j - 2).wait()

            lhs = xt[j % 2].reshape(total, tn)
            for n in range(0, ff, ff // 2):
                oin[j % 2, :, n : n + ff // 2] = lax.dot_general(
                    lhs, dpre[:, :, :, n : n + ff // 2].reshape(total, ff // 2), (((0,), (0,)), ((), ())),
                    preferred_element_type=F32,
                ).astype(BF16)
            put_in(j).start()

        get_w(0).start()
        get_dy(0).start()

        def step(s):
            step_in()
            add_core(s)
            swap(s)
            along(s, 1, first, rcopy, in_r, out_r)
            along(s, -1, last, lcopy, in_l, out_l)
            settle(s, 1, rcopy, in_r)
            settle(s, -1, lcopy, in_l)
            across(s)
            finish(s)
            move_x(s + LEAD)

            @pl.when(s < steps - WINDOW)
            def _():
                step_out()

            @pl.when(s < nt)
            def _():
                term(s)

            @pl.when(inside(s - 1))
            def _():
                xd(s - 1, 1 - c).wait_recv()
                get_x(s - 1).start()

            m = s - (s + 1) // 8

            @pl.when(((s + 1) % 8 != 0) & (m < nt))
            def _():
                down(m)

            @pl.when(inside(s - 1))
            def _():
                inward(s - 1)

        loop(steps, step)
        loop(2, lambda i: finish(steps + i))

        for j in range(nt - RING, nt):
            slot = j % RING
            for k in range(NZ - 1):
                swapped = k == 0 and j % 2 == 0

                @pl.when((z + k + 1 < NZ) & jnp.logical_not(first & swapped))
                def _():
                    rcopy(slot, k).wait_send()

                @pl.when((z - k - 1 >= 0) & jnp.logical_not(last & swapped))
                def _():
                    lcopy(slot, k).wait_send()

            if j % 2 == 0:

                @pl.when(edge)
                def _():
                    wcopy(slot).wait_send()
                    ecopy(slot, p_nxt).wait_send()

            dsum(slot).wait_send()
            ysum(slot).wait_send()
            xy(j, y).wait_send()
            xd(j, c).wait_send()
            x_out(j, 1, True)
            x_out(j, -1, True)

            @pl.when(z == 2)
            def _():
                xz(j, 1, 1, 0).wait_send()

            @pl.when(z == 1)
            def _():
                xz(j, -1, 1, NZ - 1).wait_send()

        for j in range(nt - 2, nt):
            put_dn(j).wait()
            put_in(j).wait()
            put_dx(j).wait()

    pl.run_scoped(
        phase2,
        pltpu.VMEM((OWN, NY, NZ, rows, tn), F32),
        pltpu.VMEM((RING, NZ - 1, NY, rows, tn), BF16),
        pltpu.VMEM((RING, NZ - 1, NY, rows, tn), BF16),
        pltpu.VMEM((RING, NY * NZ, rows, tn), BF16),
        pltpu.VMEM((RING, rows, tn), BF16),
        pltpu.VMEM((RING, rows, tn), BF16),
        pltpu.VMEM((RING, rows, tn), BF16),
        pltpu.VMEM((2, tn, ff), BF16),
        pltpu.VMEM((2, NY * NZ, NC, rows, tn), BF16),
        pltpu.VMEM((2, NY * NZ, NC, rows, tn), BF16),
        pltpu.VMEM((2, ff, tn), BF16),
        pltpu.VMEM((2, tn, ff), BF16),
        pltpu.VMEM((2, rows, tn), BF16),
        pltpu.SemaphoreType.DMA((6, 2)),
    )


def call(rows, d, ff, tn, nch, fn, x, dy, pre, win, wdn):
    blocks = NY * NZ
    total = blocks * NC * rows
    dma = pltpu.SemaphoreType.DMA
    any_ = pl.BlockSpec(memory_space=pl.ANY)
    return pl.pallas_call(
        functools.partial(bwd_kernel, (rows, d, ff, tn, nch, fn)),
        name="bwd",
        out_shape=[
            jax.ShapeDtypeStruct((rows, d), BF16),
            jax.ShapeDtypeStruct((d, ff), BF16),
            jax.ShapeDtypeStruct((ff, d), BF16),
            jax.ShapeDtypeStruct((blocks, NC, rows, d), BF16),
            jax.ShapeDtypeStruct((blocks, NC, rows, d), BF16),
        ],
        in_specs=[any_] * 5,
        out_specs=[any_] * 5,
        scratch_shapes=[
            pltpu.VMEM((blocks, NC, rows, ff), BF16),
            pltpu.VMEM((ff, total), BF16),
            pltpu.VMEM((RING, NZ - 1, NY, rows, tn), BF16),
            pltpu.VMEM((RING, NZ - 1, NY, rows, tn), BF16),
            pltpu.VMEM((RING, blocks, rows, tn), BF16),
            pltpu.VMEM((RING, rows, tn), BF16),
            pltpu.VMEM((RING, rows, tn), BF16),
            pltpu.VMEM((RING, rows, tn), BF16),
            dma((NZ, nch + 1)), dma((NZ, nch)), dma((blocks, nch)),
            dma((NZ, nch + 1)), dma((NZ, nch + 1)), dma((NZ, nch)), dma((blocks, nch)),
            dma((2,)), dma((2,)), dma((4,)),
            dma((RING, NZ - 1)), dma((RING, NZ - 1)), dma((RING,)), dma((RING,)), dma((RING,)), dma((RING,)),
            dma((RING, NZ - 1)), dma((RING, NZ - 1)), dma((RING,)), dma((RING,)), dma((RING,)), dma((RING,)),
            dma((2, 2, RING)), dma((2, 2, RING)), dma((RING,)), dma((RING,)), dma((RING,)), dma((RING,)),
            pltpu.SemaphoreType.REGULAR((4,)),
        ],
        compiler_params=pltpu.CompilerParams(
            collective_id=0, has_side_effects=True, vmem_limit_bytes=67043328
        ),
    )(x, dy, pre, win, wdn)


def solution(mesh):
    spec = jax.sharding.PartitionSpec
    rows_of, cols_of = spec(("dp", "tp"), None), spec("dp", "tp")

    def local(x, dy, pre, win, wdn):
        rows, d = x.shape
        ff = pre.shape[1]
        dx, dwin, dwdn, _, _ = call(rows, d, ff, 256, 7, 256, x, dy, pre, win, wdn)
        return dx, dwin, dwdn

    return jax.shard_map(
        local,
        mesh=mesh,
        in_specs=(rows_of, rows_of, cols_of, spec(None, "tp"), spec("tp", None)),
        out_specs=(rows_of, cols_of, rows_of),
        check_vma=False,
    )
```

```python
import functools

import jax
import jax.numpy as jnp
from jax import lax
from jax.experimental import pallas as pl
from jax.experimental.pallas import tpu as pltpu

MESH = pl.DeviceIdType.MESH
BF16, F32 = jnp.bfloat16, jnp.float32
NY, NZ, NC = 2, 4, 2
RING = 4
OWN = 6
WINDOW = 2
TAIL = 4
SLACK = 12.0
LEAD = 5
ROOT = 0.7978845608028654
CUBE = 0.044715


def relays(inner, n):
    block = 50.0
    chunk = block / n
    due = {}
    for q in range(n):
        here = (q + 1) * chunk
        due[0, q] = -1.0
        due[1, q] = due[2, q] = here
        due[3, q] = here if inner else block + 2 * chunk + here
        due[4, q] = block + here - chunk if q else block + 2 * chunk
        due[5, q] = 2 * block - chunk + here - chunk if q else 2.4 * chunk + (block if inner else 2 * block)
        due[6, q] = (block + 2 * chunk if inner else 2 * block + 3 * chunk) + here
        due[7, q] = 3 * block - 2 * chunk + here - chunk if q else 2.4 * chunk + (2 * block if inner else 3 * block + chunk)
    for i, q in due:
        if i in (4, 5, 7) and q:
            due[i, q] += SLACK
    order = sorted(due, key=lambda k: (due[k], k[1], k[0]))
    first, last = {}, {}
    for e, (i, _) in enumerate(order):
        first.setdefault(i, e)
        last[i] = e
    codes, keep, free = [], {}, [2, 1, 0]
    for e, (i, q) in enumerate(order):
        if e == first[i]:
            keep[i] = free.pop()
        mark = (e == first[i]) + 2 * (e == last[i])
        codes.append(((i * 16 + q) * 4 + mark) * 4 + keep[i])
        if e == last[i]:
            free.append(keep[i])
    return codes


def bwd_kernel(
    dims,
    x_ref, dy_ref, pre_ref, win_ref, wdn_ref,
    dx_ref, dwin_ref, dwdn_ref, fx_ref, fdy_ref,
    dpre, hidt, in_r, in_l, in_d, in_y, in_w, in_e,
    rz, ry, rd, szp, szm, sy, sd, rx, sx, lsem, ls1, ls2,
    r_r, r_l, r_d, r_y, r_w, r_e, s_r, s_l, s_d, s_y, s_w, s_e,
    rxz, sxz, rxy, sxy, rxd, sxd, cred,
):
    rows, d, ff, tn, nch, fn = dims
    nt = d // tn
    ck = d // nch
    total = NY * NZ * NC * rows
    t = lax.axis_index("tp")
    c = t % NC
    z = (t // NC) % NZ
    y = t // (NC * NZ)
    yz = y * NZ + z
    p_zp, p_zm = t + NC, t - NC
    p_y = ((1 - y) * NZ + z) * NC + c
    p_d = yz * NC + (1 - c)
    first, last = z == 0, z == NZ - 1

    def remote(src, dst, ssem, rsem, to):
        return pltpu.make_async_remote_copy(
            src, dst, ssem, rsem, device_id={"tp": to}, device_id_type=MESH
        )

    def signal(sem, to):
        pl.semaphore_signal(sem, inc=1, device_id={"tp": to}, device_id_type=MESH)

    def cols(j, width):
        return pl.ds(pl.multiple_of(j * width, width), width)

    def loop(n, body):
        def step(i, carry):
            body(i)
            return carry

        lax.fori_loop(0, n, step, 0)

    barrier = pltpu.get_barrier_semaphore()
    signal(barrier, p_y)
    signal(barrier, p_d)

    @pl.when(jnp.logical_not(last))
    def _():
        signal(barrier, p_zp)

    @pl.when(jnp.logical_not(first))
    def _():
        signal(barrier, p_zm)

    pl.semaphore_wait(barrier, 4 - jnp.where(first | last, 1, 0))

    inner = (z == 1) | (z == NZ - 2)
    edge = first | last

    def inside(j):
        return (j >= 0) & (j < nt)

    def xz(j, away, stage, zb, n=1):
        ref = fx_ref.at[pl.ds(y * NZ + zb, n), c, :, cols(j, tn)]
        k = 0 if away == 1 else 1
        return remote(ref, ref, sxz.at[k, stage, j % RING], rxz.at[k, stage, j % RING], p_zp if away == 1 else p_zm)

    def xy(j, row):
        ref = fx_ref.at[pl.ds(row * NZ, NZ), c, :, cols(j, tn)]
        return remote(ref, ref, sxy.at[j % RING], rxy.at[j % RING], p_y)

    def xd(j, core):
        ref = fx_ref.at[:, core, :, cols(j, tn)]
        return remote(ref, ref, sxd.at[j % RING], rxd.at[j % RING], p_d)

    def send(j, make):
        @pl.when(j >= RING)
        def _():
            make(j - RING).wait_send()

        make(j).start()

    def x_out(j, away, wait=False):
        end = 2 if away == 1 else 1

        def do(make):
            if wait:
                make(j).wait_send()
            else:
                send(j, make)

        @pl.when(z == end)
        def _():
            do(lambda i: xz(i, away, 0, 1, 2))

        @pl.when(z == NZ - 1 - end)
        def _():
            do(lambda i: xz(i, away, 0, 0 if away == 1 else NZ - 1))

    def move_x(s):
        @pl.when(inside(s))
        def _():
            x_out(s, 1)
            x_out(s, -1)

        @pl.when(inside(s - 2))
        def _():
            j = s - 2

            @pl.when(last)
            def _():
                xz(j, 1, 0, 1, 2).wait_recv()

            @pl.when(first)
            def _():
                xz(j, -1, 0, 1, 2).wait_recv()

            @pl.when(z == 2)
            def _():
                xz(j, 1, 0, 0).wait_recv()
                send(j, lambda i: xz(i, 1, 1, 0))

            @pl.when(z == 1)
            def _():
                xz(j, -1, 0, NZ - 1).wait_recv()
                send(j, lambda i: xz(i, -1, 1, NZ - 1))

        @pl.when(inside(s - 4))
        def _():
            j = s - 4

            @pl.when(last)
            def _():
                xz(j, 1, 1, 0).wait_recv()

            @pl.when(first)
            def _():
                xz(j, -1, 1, NZ - 1).wait_recv()

            send(j, lambda i: xy(i, y))

        @pl.when(inside(s - 6))
        def _():
            xy(s - 6, 1 - y).wait_recv()
            send(s - 6, lambda i: xd(i, c))

    def step_in():
        pl.semaphore_wait(cred.at[2], 1)
        pl.semaphore_wait(cred.at[3], 1)

        @pl.when(jnp.logical_not(last))
        def _():
            pl.semaphore_wait(cred.at[0], 1)

        @pl.when(jnp.logical_not(first))
        def _():
            pl.semaphore_wait(cred.at[1], 1)

    def step_out():
        signal(cred.at[2], p_y)
        signal(cred.at[3], p_d)

        @pl.when(jnp.logical_not(last))
        def _():
            signal(cred.at[1], p_zp)

        @pl.when(jnp.logical_not(first))
        def _():
            signal(cred.at[0], p_zm)

    def dy_at(b, core, q):
        return fdy_ref.at[b, core, :, cols(q, ck)]

    def zcopy(row, zb, q, away, src=None):
        ref = dy_at(row * NZ + zb, c, q)
        back = row != y
        rsem = rz.at[zb, jnp.where(back, nch, q)]
        if away == 1:
            return remote(ref if src is None else src, ref, szp.at[zb, jnp.where(back, nch, q)], rsem, p_zp)
        return remote(ref if src is None else src, ref, szm.at[zb, jnp.where(back, nch, q)], rsem, p_zm)

    def ycopy(row, zb, q, src=None):
        ref = dy_at(row * NZ + zb, c, q)
        return remote(ref if src is None else src, ref, sy.at[zb, q], ry.at[zb, q], p_y)

    def dcopy(b, core, q, src=None):
        ref = dy_at(b, core, q)
        return remote(ref if src is None else src, ref, sd.at[b, q], rd.at[b, q], p_d)

    def xcopy(k, to, b):
        return remote(x_ref, fx_ref.at[b, c], sx.at[k], rx.at[k], to)

    def phase1(wdn):
        w_load = pltpu.make_async_copy(wdn_ref, wdn, lsem.at[0])

        def start(bounce, part_of_pre):
            own_dy = pltpu.make_async_copy(dy_ref, bounce.at[0], lsem.at[1])
            own_x = pltpu.make_async_copy(x_ref, bounce.at[1], lsem.at[2])
            own_dy.start()
            own_x.start()

            def send_own(q):
                src = dy_ref.at[:, cols(q, ck)]

                @pl.when(jnp.logical_not(last))
                def _():
                    zcopy(y, z, q, 1, src).start()

                @pl.when(jnp.logical_not(first))
                def _():
                    zcopy(y, z, q, -1, src).start()

                ycopy(y, z, q, src).start()
                dcopy(yz, c, q, src).start()

            loop(nch, send_own)

            hr = part_of_pre.shape[1]

            def get(r):
                return pltpu.make_async_copy(
                    pre_ref.at[pl.ds(pl.multiple_of(r * hr, hr), hr)], part_of_pre.at[r % 2], ls1.at[r % 2]
                )

            get(0).start()
            own_dy.wait()
            own_x.wait()
            put_dy = pltpu.make_async_copy(bounce.at[0], fdy_ref.at[yz, c], lsem.at[1])
            put_x = pltpu.make_async_copy(bounce.at[1], fx_ref.at[yz, c], lsem.at[2])
            put_dy.start()
            put_x.start()
            w_load.start()

            def hidden(r):
                get(r).wait()

                @pl.when(r + 1 < total // hr)
                def _():
                    get(r + 1).start()

                def part(n):
                    p = part_of_pre[r % 2, :, cols(n, hw)].astype(F32)
                    th = jnp.tanh(ROOT * (p + CUBE * (p * p * p)))
                    h = (p * (0.5 * (1.0 + th))).astype(BF16)
                    hidt[cols(n, hw), cols(r, hr)] = h.T

                hw = 256 if ff % 256 == 0 else 128
                loop(ff // hw, part)

            loop(total // hr, hidden)
            put_dy.wait()
            put_x.wait()

        pl.run_scoped(
            start, pltpu.VMEM((2, rows, d), BF16), pltpu.VMEM((2, 256 if total % 256 == 0 else 128, ff), BF16)
        )
        w_load.wait()

        o1 = jnp.where(z == 0, 1, z - 1)
        o2 = jnp.where(z == NZ - 1, 1, jnp.where(z == 2, 3, 2))
        o3 = jnp.where(z < 2, 3, 0)

        def pass_z(row, zb, q):
            @pl.when((zb < z) & (z < NZ - 1))
            def _():
                zcopy(row, zb, q, 1).start()

            @pl.when((zb > z) & (z > 0))
            def _():
                zcopy(row, zb, q, -1).start()

        def chip(i):
            row = jnp.where((i == 0) | (i == 1) | (i == 3) | (i == 6), y, 1 - y)
            near = jnp.where((i == 0) | (i == 2), z, o1)
            return row, jnp.where(i > 5, o3, jnp.where((i == 3) | (i == 5), o2, near))

        def unpack(code):
            return code // 256, code // 16 % 16, code // 4 % 4, code % 4

        def relay(code):
            i, q, _, _ = unpack(code)
            row, zb = chip(i)

            @pl.when((i > 0) & (row == y))
            def _():
                zcopy(y, zb, q, 1).wait_recv()
                pass_z(y, zb, q)

                @pl.when(q > 0)
                def _():
                    ycopy(y, zb, q).start()

            @pl.when((row != y) & (q == 0) & (i == 2))
            def _():
                ycopy(1 - y, z, 0).wait_recv()

                @pl.when(jnp.logical_not(last))
                def _():
                    zcopy(1 - y, z, 0, 1).start()

                @pl.when(jnp.logical_not(first))
                def _():
                    zcopy(1 - y, z, 0, -1).start()

                @pl.when(first)
                def _():
                    xcopy(0, p_zp, yz).start()

                @pl.when(last)
                def _():
                    xcopy(1, p_zm, yz).start()

            @pl.when((row != y) & (q == 0) & (i != 2))
            def _():
                zcopy(1 - y, zb, 0, 1).wait_recv()
                pass_z(1 - y, zb, 0)

                @pl.when((i == 4) & (z == 1))
                def _():
                    xcopy(0, p_zp, yz).start()

                @pl.when((i == 5) & (z == 2))
                def _():
                    xcopy(1, p_zm, yz).start()

            @pl.when((row != y) & (q > 0))
            def _():
                @pl.when((i == 7) & (q == nch - 3 + (nch < 4)))
                def _():
                    @pl.when(inner)
                    def _():
                        xcopy(0, p_zp, yz - 1).wait_recv()
                        xcopy(1, p_zm, yz + 1).wait_recv()

                    for v in range(WINDOW):
                        move_x(v)
                        step_out()

                ycopy(1 - y, zb, q).wait_recv()

            @pl.when(i > 0)
            def _():
                dcopy(row * NZ + zb, c, q).start()

            @pl.when((i == 7) & (q == nch - 1))
            def _():
                for v in range(WINDOW, LEAD - 1):
                    step_in()
                    move_x(v)
                    step_out()

        def stream(dyc, preu, acc):
            orders = [[relays(inner_chip, nch)[e] for e in range(NY * NZ * nch)] for inner_chip in (False, True)]
            places = len(orders[0])

            def at(e):
                code = jnp.where(inner, orders[1][0], orders[0][0])
                for k in range(1, places):
                    code = jnp.where(e == k, jnp.where(inner, orders[1][k], orders[0][k]), code)
                return code

            def get(code, slot):
                i, q, _, _ = unpack(code)
                row, zb = chip(i)
                return pltpu.make_async_copy(
                    fdy_ref.at[row * NZ + zb, :, :, cols(q, ck)], dyc.at[slot], ls1.at[slot]
                )

            def fetch(code, slot):
                i, q, _, _ = unpack(code)
                row, zb = chip(i)
                dcopy(row * NZ + zb, 1 - c, q).wait_recv()
                get(code, slot).start()

            def get_pre(u, keep):
                at = pl.ds(pl.multiple_of(u * (NC * rows), NC * rows), NC * rows)
                return pltpu.make_async_copy(pre_ref.at[at], preu.at[keep], ls2.at[keep])

            def place(e, codes):
                code, following = codes
                later = at(e + 2)

                @pl.when(e + 2 < places)
                def _():
                    relay(later)

                @pl.when(e + 1 < places)
                def _():
                    fetch(following, (e + 1) % 2)

                i, q, mark, keep = unpack(code)
                row, zb = chip(i)
                u = row * NZ + zb

                @pl.when(mark % 2 == 1)
                def _():
                    get_pre(u, keep).start()

                get(code, e % 2).wait()
                lhs = dyc[e % 2].reshape(NC * rows, ck)
                for n in range(0, ff, fn):
                    term = lax.dot_general(
                        lhs, wdn[n : n + fn, cols(q, ck)], (((1,), (1,)), ((), ())), preferred_element_type=F32
                    )
                    acc[keep, :, n : n + fn] = jnp.where(mark % 2 == 1, 0.0, acc[keep, :, n : n + fn]) + term

                @pl.when(mark >= 2)
                def _():
                    get_pre(u, keep).wait()

                    def part(n):
                        p = preu[keep, :, cols(n, fn)].astype(F32)
                        pp = p * p
                        th = jnp.tanh(ROOT * (p + CUBE * (p * pp)))
                        slope = 0.5 * (1.0 + th) + (0.5 * p) * (1.0 - th * th) * (ROOT * (1.0 + 3.0 * CUBE * pp))
                        dpre[u, :, :, cols(n, fn)] = (acc[keep, :, cols(n, fn)] * slope).astype(BF16).reshape(NC, rows, fn)

                    loop(ff // fn, part)

                return following, later

            codes = at(0), at(1)
            relay(codes[0])
            relay(codes[1])
            fetch(codes[0], 0)
            lax.fori_loop(0, places, place, codes)

        pl.run_scoped(
            stream,
            pltpu.VMEM((2, NC, rows, ck), BF16),
            pltpu.VMEM((3, NC * rows, ff), BF16),
            pltpu.VMEM((3, NC * rows, ff), F32),
        )

    pl.run_scoped(phase1, pltpu.VMEM((ff, d), BF16))

    def all_sent():
        def sent(q):
            def block(zb):
                @pl.when((zb <= z) & (z < NZ - 1))
                def _():
                    zcopy(y, zb, q, 1).wait_send()

                @pl.when((zb >= z) & (z > 0))
                def _():
                    zcopy(y, zb, q, -1).wait_send()

                @pl.when(q == 0)
                def _():
                    @pl.when((zb <= z) & (z < NZ - 1))
                    def _():
                        zcopy(1 - y, zb, q, 1).wait_send()

                    @pl.when((zb >= z) & (z > 0))
                    def _():
                        zcopy(1 - y, zb, q, -1).wait_send()

                @pl.when((q > 0) | (zb == z))
                def _():
                    ycopy(y, zb, q).wait_send()

            loop(NZ, block)
            loop(NY * NZ, lambda b: dcopy(b, c, q).wait_send())

        loop(nch, sent)

        @pl.when(z < 2)
        def _():
            xcopy(0, p_zp, yz).wait_send()

        @pl.when(z >= 2)
        def _():
            xcopy(1, p_zm, yz).wait_send()

    def phase2(own, out_r, out_l, out_d, out_y, out_w, out_e, wt, dyt, xt, odn, oin, odx, ls):
        steps = nt + TAIL

        def rcopy(slot, k):
            return remote(out_r.at[slot, k], in_r.at[slot, k], s_r.at[slot, k], r_r.at[slot, k], p_zp)

        def lcopy(slot, k):
            return remote(out_l.at[slot, k], in_l.at[slot, k], s_l.at[slot, k], r_l.at[slot, k], p_zm)

        def dsum(slot):
            return remote(out_d.at[slot], in_d.at[slot], s_d.at[slot], r_d.at[slot], p_d)

        def ysum(slot):
            return remote(out_y.at[slot], in_y.at[slot], s_y.at[slot], r_y.at[slot], p_y)

        def add_core(s):
            j = s - 1

            @pl.when(inside(j))
            def _():
                slot, ring = j % RING, j % OWN
                dsum(slot).wait_recv()

                def piece(b):
                    own[ring, b // NZ, b % NZ] += in_d[slot, b].astype(F32)

                loop(NY * NZ, piece)

        def along(s, away, start, copy, inb, outb):
            behind = z if away == 1 else NZ - 1 - z
            j = s - 1 - behind

            @pl.when(inside(j))
            def _():
                slot, ring = j % RING, j % OWN
                swaps = j % 2 == 0
                for k in range(NZ - 1, 0, -1):
                    zz = z + away * k
                    here = (zz >= 0) & (zz < NZ)
                    if k == 1:
                        here = here & jnp.logical_not(start & swaps)

                    @pl.when(here)
                    def _():
                        @pl.when(j >= RING)
                        def _():
                            copy(slot, k - 1).wait_send()

                        @pl.when(start)
                        def _():
                            def piece(h):
                                outb[slot, k - 1, h] = own[ring, h, zz].astype(BF16)

                            loop(NY, piece)

                        if k < NZ - 1:

                            @pl.when(jnp.logical_not(start))
                            def _():
                                copy(slot, k).wait_recv()

                                def piece(h):
                                    outb[slot, k - 1, h] = (own[ring, h, zz] + inb[slot, k, h].astype(F32)).astype(BF16)

                                loop(NY, piece)

                        copy(slot, k - 1).start()

        def settle(s, away, copy, inb):
            behind = z if away == 1 else NZ - 1 - z
            j = s - behind - jnp.where(behind == NZ - 1, 1, 2)

            @pl.when(inside(j) & ((behind > 1) | ((behind == 1) & (j % 2 == 1))))
            def _():
                slot, ring = j % RING, j % OWN
                copy(slot, 0).wait_recv()

                def piece(h):
                    own[ring, h, z] += inb[slot, 0, h].astype(F32)

                loop(NY, piece)

        nxt = jnp.where(first, 1, NZ - 2)
        p_nxt = jnp.where(first, p_zp, p_zm)
        p_end = jnp.where(z == 1, p_zm, p_zp)

        def wcopy(slot):
            return remote(out_w.at[slot], in_w.at[slot], s_w.at[slot], r_w.at[slot], p_y)

        def ecopy(slot, to):
            return remote(out_e.at[slot], in_e.at[slot], s_e.at[slot], r_e.at[slot], to)

        def swap(s):
            def at(j, where, body):
                @pl.when(inside(j) & (j % 2 == 0) & where)
                def _():
                    body(j % RING, j % OWN, j >= RING)

            def give(slot, ring, again):
                @pl.when(again)
                def _():
                    wcopy(slot).wait_send()

                out_w[slot] = own[ring, 1 - y, nxt].astype(BF16)
                wcopy(slot).start()

            def join(slot, ring, again):
                @pl.when(again)
                def _():
                    ecopy(slot, p_nxt).wait_send()

                wcopy(slot).wait_recv()
                out_e[slot] = (own[ring, y, nxt] + in_w[slot].astype(F32)).astype(BF16)
                ecopy(slot, p_nxt).start()

            def take(slot, ring, again):
                ecopy(slot, p_end).wait_recv()
                own[ring, y, z] += in_e[slot].astype(F32)

            at(s - 1, edge, give)
            at(s - 3, edge, join)
            at(s - 4, inner, take)

        def across(s):
            j = s - 4

            @pl.when(inside(j))
            def _():
                slot, ring = j % RING, j % OWN

                @pl.when(j >= RING)
                def _():
                    ysum(slot).wait_send()

                out_y[slot] = own[ring, 1 - y, z].astype(BF16)
                ysum(slot).start()

        def put_dx(j):
            return pltpu.make_async_copy(odx.at[j % 2], dx_ref.at[:, cols(j, tn)], ls.at[5, j % 2])

        def finish(s):
            j = s - 6

            @pl.when(inside(j))
            def _():
                slot, ring = j % RING, j % OWN

                @pl.when(j >= 2)
                def _():
                    put_dx(j - 2).wait()

                ysum(slot).wait_recv()
                odx[j % 2] = (own[ring, y, z] + in_y[slot].astype(F32)).astype(BF16)
                put_dx(j).start()

        def get_x(j):
            return pltpu.make_async_copy(fx_ref.at[:, :, :, cols(j, tn)], xt.at[j % 2], ls.at[2, j % 2])

        def get_w(j):
            return pltpu.make_async_copy(win_ref.at[cols(j, tn)], wt.at[j % 2], ls.at[0, j % 2])

        def get_dy(j):
            return pltpu.make_async_copy(fdy_ref.at[:, :, :, cols(j, tn)], dyt.at[j % 2], ls.at[1, j % 2])

        def put_dn(j):
            return pltpu.make_async_copy(odn.at[j % 2], dwdn_ref.at[:, cols(j, tn)], ls.at[3, j % 2])

        def put_in(j):
            return pltpu.make_async_copy(oin.at[j % 2], dwin_ref.at[cols(j, tn)], ls.at[4, j % 2])

        def term(j):
            slot, ring = j % RING, j % OWN
            get_w(j).wait()

            @pl.when(j + 1 < nt)
            def _():
                get_w(j + 1).start()

            @pl.when(j >= RING)
            def _():
                dsum(slot).wait_send()

            def dot(core, h):
                lhs = dpre[h * NZ : (h + 1) * NZ, core].reshape(NZ * rows, ff)
                return lax.dot_general(
                    lhs, wt[j % 2], (((1,), (1,)), ((), ())), preferred_element_type=F32
                ).reshape(NZ, rows, tn)

            for h in range(NY):
                out_d[slot, h * NZ : (h + 1) * NZ] = dot(1 - c, h).astype(BF16)
            dsum(slot).start()
            for h in range(NY):
                own[ring, h] = dot(c, h)

        def down(j):
            get_dy(j).wait()

            @pl.when(j + 1 < nt)
            def _():
                get_dy(j + 1).start()

            @pl.when(j >= 2)
            def _():
                put_dn(j - 2).wait()

            rhs = dyt[j % 2].reshape(total, tn)
            for m in range(0, ff, ff // 4):
                odn[j % 2, m : m + ff // 4] = jnp.dot(
                    hidt[m : m + ff // 4], rhs, preferred_element_type=F32
                ).astype(BF16)
            put_dn(j).start()

        def inward(j):
            get_x(j).wait()

            @pl.when(j >= 2)
            def _():
                put_in(j - 2).wait()

            lhs = xt[j % 2].reshape(total, tn)
            for n in range(0, ff, ff // 2):
                oin[j % 2, :, n : n + ff // 2] = lax.dot_general(
                    lhs, dpre[:, :, :, n : n + ff // 2].reshape(total, ff // 2), (((0,), (0,)), ((), ())),
                    preferred_element_type=F32,
                ).astype(BF16)
            put_in(j).start()

        get_w(0).start()
        get_dy(0).start()

        step_in()
        move_x(LEAD - 1)
        step_out()

        def step(s):
            step_in()
            add_core(s)
            swap(s)
            along(s, 1, first, rcopy, in_r, out_r)
            along(s, -1, last, lcopy, in_l, out_l)
            settle(s, 1, rcopy, in_r)
            settle(s, -1, lcopy, in_l)
            across(s)
            finish(s)
            move_x(s + LEAD)

            @pl.when(s < steps - WINDOW)
            def _():
                step_out()

            @pl.when(s < nt)
            def _():
                term(s)

            @pl.when(s == nt + 1)
            def _():
                all_sent()

            @pl.when(inside(s - 1))
            def _():
                xd(s - 1, 1 - c).wait_recv()
                get_x(s - 1).start()

            m = s - s // 9 - 1

            @pl.when((s % 9 != 0) & (m < nt))
            def _():
                down(m)

            @pl.when(inside(s - 1))
            def _():
                inward(s - 1)

        loop(steps, step)
        loop(2, lambda i: finish(steps + i))

        for j in range(nt - RING, nt):
            slot = j % RING
            for k in range(NZ - 1):
                swapped = k == 0 and j % 2 == 0

                @pl.when((z + k + 1 < NZ) & jnp.logical_not(first & swapped))
                def _():
                    rcopy(slot, k).wait_send()

                @pl.when((z - k - 1 >= 0) & jnp.logical_not(last & swapped))
                def _():
                    lcopy(slot, k).wait_send()

            if j % 2 == 0:

                @pl.when(edge)
                def _():
                    wcopy(slot).wait_send()
                    ecopy(slot, p_nxt).wait_send()

            dsum(slot).wait_send()
            ysum(slot).wait_send()
            xy(j, y).wait_send()
            xd(j, c).wait_send()
            x_out(j, 1, True)
            x_out(j, -1, True)

            @pl.when(z == 2)
            def _():
                xz(j, 1, 1, 0).wait_send()

            @pl.when(z == 1)
            def _():
                xz(j, -1, 1, NZ - 1).wait_send()

        for j in range(nt - 2, nt):
            put_dn(j).wait()
            put_in(j).wait()
            put_dx(j).wait()

    pl.run_scoped(
        phase2,
        pltpu.VMEM((OWN, NY, NZ, rows, tn), F32),
        pltpu.VMEM((RING, NZ - 1, NY, rows, tn), BF16),
        pltpu.VMEM((RING, NZ - 1, NY, rows, tn), BF16),
        pltpu.VMEM((RING, NY * NZ, rows, tn), BF16),
        pltpu.VMEM((RING, rows, tn), BF16),
        pltpu.VMEM((RING, rows, tn), BF16),
        pltpu.VMEM((RING, rows, tn), BF16),
        pltpu.VMEM((2, tn, ff), BF16),
        pltpu.VMEM((2, NY * NZ, NC, rows, tn), BF16),
        pltpu.VMEM((2, NY * NZ, NC, rows, tn), BF16),
        pltpu.VMEM((2, ff, tn), BF16),
        pltpu.VMEM((2, tn, ff), BF16),
        pltpu.VMEM((2, rows, tn), BF16),
        pltpu.SemaphoreType.DMA((6, 2)),
    )


def call(rows, d, ff, tn, nch, fn, x, dy, pre, win, wdn):
    blocks = NY * NZ
    total = blocks * NC * rows
    dma = pltpu.SemaphoreType.DMA
    any_ = pl.BlockSpec(memory_space=pl.ANY)
    return pl.pallas_call(
        functools.partial(bwd_kernel, (rows, d, ff, tn, nch, fn)),
        name="bwd",
        out_shape=[
            jax.ShapeDtypeStruct((rows, d), BF16),
            jax.ShapeDtypeStruct((d, ff), BF16),
            jax.ShapeDtypeStruct((ff, d), BF16),
            jax.ShapeDtypeStruct((blocks, NC, rows, d), BF16),
            jax.ShapeDtypeStruct((blocks, NC, rows, d), BF16),
        ],
        in_specs=[any_] * 5,
        out_specs=[any_] * 5,
        scratch_shapes=[
            pltpu.VMEM((blocks, NC, rows, ff), BF16),
            pltpu.VMEM((ff, total), BF16),
            pltpu.VMEM((RING, NZ - 1, NY, rows, tn), BF16),
            pltpu.VMEM((RING, NZ - 1, NY, rows, tn), BF16),
            pltpu.VMEM((RING, blocks, rows, tn), BF16),
            pltpu.VMEM((RING, rows, tn), BF16),
            pltpu.VMEM((RING, rows, tn), BF16),
            pltpu.VMEM((RING, rows, tn), BF16),
            dma((NZ, nch + 1)), dma((NZ, nch)), dma((blocks, nch)),
            dma((NZ, nch + 1)), dma((NZ, nch + 1)), dma((NZ, nch)), dma((blocks, nch)),
            dma((2,)), dma((2,)), dma((3,)), dma((2,)), dma((3,)),
            dma((RING, NZ - 1)), dma((RING, NZ - 1)), dma((RING,)), dma((RING,)), dma((RING,)), dma((RING,)),
            dma((RING, NZ - 1)), dma((RING, NZ - 1)), dma((RING,)), dma((RING,)), dma((RING,)), dma((RING,)),
            dma((2, 2, RING)), dma((2, 2, RING)), dma((RING,)), dma((RING,)), dma((RING,)), dma((RING,)),
            pltpu.SemaphoreType.REGULAR((4,)),
        ],
        compiler_params=pltpu.CompilerParams(
            collective_id=0, has_side_effects=True, vmem_limit_bytes=67043328
        ),
    )(x, dy, pre, win, wdn)


def solution(mesh):
    spec = jax.sharding.PartitionSpec
    rows_of, cols_of = spec(("dp", "tp"), None), spec("dp", "tp")

    def local(x, dy, pre, win, wdn):
        rows, d = x.shape
        ff = pre.shape[1]
        dx, dwin, dwdn, _, _ = call(rows, d, ff, 256, 7, 256, x, dy, pre, win, wdn)
        return dx, dwin, dwdn

    return jax.shard_map(
        local,
        mesh=mesh,
        in_specs=(rows_of, rows_of, cols_of, spec(None, "tp"), spec("tp", None)),
        out_specs=(rows_of, cols_of, rows_of),
        check_vma=False,
    )
```

```python
import functools

import jax
import jax.numpy as jnp
from jax import lax
from jax.experimental import pallas as pl
from jax.experimental.pallas import tpu as pltpu

MESH = pl.DeviceIdType.MESH
BF16, F32 = jnp.bfloat16, jnp.float32
NY, NZ, NC = 2, 4, 2
RING = 4
OWN = 6
DRING = 3
WINDOW = 2
TAIL = 4
SLACK = 12.0
LEAD = 5
ROOT = 0.7978845608028654
CUBE = 0.044715
END = NZ - 1
ROW_BY_ROW = (((1,), (1,)), ((), ()))


def relays(inner, n):
    block = 50.0
    chunk = block / n
    due = {}
    for q in range(n):
        here = (q + 1) * chunk
        due[0, q] = -1.0
        due[1, q] = due[2, q] = here
        due[3, q] = here if inner else block + 2 * chunk + here
        due[4, q] = block + here - chunk if q else block + 2 * chunk
        due[5, q] = 2 * block - chunk + here - chunk if q else 2.4 * chunk + (block if inner else 2 * block)
        due[6, q] = (block + 2 * chunk if inner else 2 * block + 3 * chunk) + here
        due[7, q] = 3 * block - 2 * chunk + here - chunk if q else 2.4 * chunk + (2 * block if inner else 3 * block + chunk)
    for i, q in due:
        if i in (4, 5, 7) and q:
            due[i, q] += SLACK
    order = sorted(due, key=lambda k: (due[k], k[1], k[0]))
    first, last = {}, {}
    for e, (i, _) in enumerate(order):
        first.setdefault(i, e)
        last[i] = e
    codes, keep, free = [], {}, [2, 1, 0]
    for e, (i, q) in enumerate(order):
        if e == first[i]:
            keep[i] = free.pop()
        mark = (e == first[i]) + 2 * (e == last[i])
        codes.append(((i * 16 + q) * 4 + mark) * 4 + keep[i])
        if e == last[i]:
            free.append(keep[i])
    return codes


def bwd_kernel(
    dims,
    x_ref, dy_ref, pre_ref, win_ref, wdn_ref,
    dx_ref, dwin_ref, dwdn_ref, fx_ref, fdy_ref, fe_ref,
    dpre, hidt, in_r, in_l, in_d, in_y,
    rz, ry, rd, szp, szm, sy, sd, rx, sx, lsem, ls1, ls2, ls3,
    r_r, r_l, r_d, r_y, r_ed, r_ez, s_r, s_l, s_d, s_y, s_ed, s_ez,
    rxz, sxz, rxy, sxy, rxd, sxd, cred,
):
    rows, d, ff, tn, nch, fn = dims
    nt = d // tn
    ck = d // nch
    total = NY * NZ * NC * rows
    t = lax.axis_index("tp")
    c = t % NC
    z = (t // NC) % NZ
    y = t // (NC * NZ)
    yz = y * NZ + z
    other_y, other_c = 1 - y, 1 - c
    p_zp, p_zm = t + NC, t - NC
    p_y = (other_y * NZ + z) * NC + c
    p_d = yz * NC + other_c
    first, last = z == 0, z == END

    def remote(src, dst, ssem, rsem, to):
        return pltpu.make_async_remote_copy(
            src, dst, ssem, rsem, device_id={"tp": to}, device_id_type=MESH
        )

    def signal(sem, to):
        pl.semaphore_signal(sem, inc=1, device_id={"tp": to}, device_id_type=MESH)

    def cols(j, width):
        return pl.ds(pl.multiple_of(j * width, width), width)

    def loop(n, body):
        def step(i, carry):
            body(i)
            return carry

        lax.fori_loop(0, n, step, 0)

    barrier = pltpu.get_barrier_semaphore()
    signal(barrier, p_y)
    signal(barrier, p_d)

    @pl.when(jnp.logical_not(last))
    def _():
        signal(barrier, p_zp)

    @pl.when(jnp.logical_not(first))
    def _():
        signal(barrier, p_zm)

    pl.semaphore_wait(barrier, 4 - jnp.where(first | last, 1, 0))

    inner = (z == 1) | (z == NZ - 2)
    edge = first | last

    def inside(j):
        return (j >= 0) & (j < nt)

    def xz(j, away, stage, zb, n=1):
        ref = fx_ref.at[pl.ds(y * NZ + zb, n), c, :, cols(j, tn)]
        k = 0 if away == 1 else 1
        return remote(ref, ref, sxz.at[k, stage, j % RING], rxz.at[k, stage, j % RING], p_zp if away == 1 else p_zm)

    def xy(j, row):
        ref = fx_ref.at[pl.ds(row * NZ, NZ), c, :, cols(j, tn)]
        return remote(ref, ref, sxy.at[j % RING], rxy.at[j % RING], p_y)

    def xd(j, core):
        ref = fx_ref.at[:, core, :, cols(j, tn)]
        return remote(ref, ref, sxd.at[j % RING], rxd.at[j % RING], p_d)

    def send(j, make):
        @pl.when(j >= RING)
        def _():
            make(j - RING).wait_send()

        make(j).start()

    def x_out(j, away, wait=False):
        end = 2 if away == 1 else 1

        def do(make):
            if wait:
                make(j).wait_send()
            else:
                send(j, make)

        @pl.when(z == end)
        def _():
            do(lambda i: xz(i, away, 0, 1, 2))

        @pl.when(z == END - end)
        def _():
            do(lambda i: xz(i, away, 0, 0 if away == 1 else END))

    def move_x(s):
        @pl.when(inside(s))
        def _():
            x_out(s, 1)
            x_out(s, -1)

        @pl.when(inside(s - 2))
        def _():
            j = s - 2

            @pl.when(last)
            def _():
                xz(j, 1, 0, 1, 2).wait_recv()

            @pl.when(first)
            def _():
                xz(j, -1, 0, 1, 2).wait_recv()

            @pl.when(z == 2)
            def _():
                xz(j, 1, 0, 0).wait_recv()
                send(j, lambda i: xz(i, 1, 1, 0))

            @pl.when(z == 1)
            def _():
                xz(j, -1, 0, END).wait_recv()
                send(j, lambda i: xz(i, -1, 1, END))

        @pl.when(inside(s - 4))
        def _():
            j = s - 4

            @pl.when(last)
            def _():
                xz(j, 1, 1, 0).wait_recv()

            @pl.when(first)
            def _():
                xz(j, -1, 1, END).wait_recv()

            send(j, lambda i: xy(i, y))

        @pl.when(inside(s - 6))
        def _():
            xy(s - 6, other_y).wait_recv()
            send(s - 6, lambda i: xd(i, c))

    def step_in():
        pl.semaphore_wait(cred.at[2], 1)
        pl.semaphore_wait(cred.at[3], 1)

        @pl.when(jnp.logical_not(last))
        def _():
            pl.semaphore_wait(cred.at[0], 1)

        @pl.when(jnp.logical_not(first))
        def _():
            pl.semaphore_wait(cred.at[1], 1)

    def step_out():
        signal(cred.at[2], p_y)
        signal(cred.at[3], p_d)

        @pl.when(jnp.logical_not(last))
        def _():
            signal(cred.at[1], p_zp)

        @pl.when(jnp.logical_not(first))
        def _():
            signal(cred.at[0], p_zm)

    nearly = (nt + 1) // 2
    nxt = jnp.where(first, 1, NZ - 2)
    p_nxt = jnp.where(first, p_zp, p_zm)

    def edcopy(out, r):
        return remote(out.at[r % 2], in_d.at[r % DRING, pl.ds(0, NY)], s_ed.at[r % 2], r_ed.at[r % DRING], p_d)

    def ezcopy(r, out=None):
        src = fe_ref.at[r] if out is None else out.at[r % 2]
        return remote(src, fe_ref.at[r], s_ez.at[r % 2], r_ez.at[r], p_nxt)

    def early_step(r, wte, e_d, e_own, e_out):
        def get_w(i):
            return pltpu.make_async_copy(win_ref.at[cols(2 * i, tn)], wte, ls3.at[0])

        @pl.when((r >= 1) & (r <= nearly))
        def _():
            k = r - 1

            @pl.when(k >= 2)
            def _():
                ezcopy(k - 2, e_out).wait_send()

            edcopy(e_d, k).wait_recv()
            e_out[k % 2] = (e_own[k % 2] + in_d[k % DRING, :NY].astype(F32)).astype(BF16)
            ezcopy(k, e_out).start()

        @pl.when(r == -1)
        def _():
            get_w(0).start()

        @pl.when((r >= 0) & (r < nearly))
        def _():
            get_w(r).wait()

            @pl.when(r >= 2)
            def _():
                edcopy(e_d, r - 2).wait_send()

            def dot(core, h):
                return lax.dot_general(
                    dpre[h * NZ + nxt, core], wte[...], ROW_BY_ROW, preferred_element_type=F32
                )

            for h in range(NY):
                e_d[r % 2, h] = dot(other_c, h).astype(BF16)
            edcopy(e_d, r).start()
            for h in range(NY):
                e_own[r % 2, h] = dot(c, h)

            @pl.when(r + 1 < nearly)
            def _():
                get_w(r + 1).start()

    def dy_at(b, core, q):
        return fdy_ref.at[b, core, :, cols(q, ck)]

    def zcopy(row, zb, q, away, src=None):
        ref = dy_at(row * NZ + zb, c, q)
        back = row != y
        rsem = rz.at[zb, jnp.where(back, nch, q)]
        if away == 1:
            return remote(ref if src is None else src, ref, szp.at[zb, jnp.where(back, nch, q)], rsem, p_zp)
        return remote(ref if src is None else src, ref, szm.at[zb, jnp.where(back, nch, q)], rsem, p_zm)

    def ycopy(row, zb, q, src=None):
        ref = dy_at(row * NZ + zb, c, q)
        return remote(ref if src is None else src, ref, sy.at[zb, q], ry.at[zb, q], p_y)

    def dcopy(b, core, q, src=None):
        ref = dy_at(b, core, q)
        return remote(ref if src is None else src, ref, sd.at[b, q], rd.at[b, q], p_d)

    def xcopy(k, to, b):
        return remote(x_ref, fx_ref.at[b, c], sx.at[k], rx.at[k], to)

    def phase1(wdn):
        w_load = pltpu.make_async_copy(wdn_ref, wdn, lsem.at[0])

        def start(bounce, part_of_pre):
            own_dy = pltpu.make_async_copy(dy_ref, bounce.at[0], lsem.at[1])
            own_x = pltpu.make_async_copy(x_ref, bounce.at[1], lsem.at[2])
            own_dy.start()
            own_x.start()

            def send_own(q):
                src = dy_ref.at[:, cols(q, ck)]

                @pl.when(jnp.logical_not(last))
                def _():
                    zcopy(y, z, q, 1, src).start()

                @pl.when(jnp.logical_not(first))
                def _():
                    zcopy(y, z, q, -1, src).start()

                ycopy(y, z, q, src).start()
                dcopy(yz, c, q, src).start()

            loop(nch, send_own)

            hr = part_of_pre.shape[1]

            def get(r):
                return pltpu.make_async_copy(
                    pre_ref.at[pl.ds(pl.multiple_of(r * hr, hr), hr)], part_of_pre.at[r % 2], ls1.at[r % 2]
                )

            get(0).start()
            own_dy.wait()
            own_x.wait()
            put_dy = pltpu.make_async_copy(bounce.at[0], fdy_ref.at[yz, c], lsem.at[1])
            put_x = pltpu.make_async_copy(bounce.at[1], fx_ref.at[yz, c], lsem.at[2])
            put_dy.start()
            put_x.start()
            w_load.start()

            def hidden(r):
                get(r).wait()

                @pl.when(r + 1 < total // hr)
                def _():
                    get(r + 1).start()

                def part(n):
                    p = part_of_pre[r % 2, :, cols(n, hw)].astype(F32)
                    th = jnp.tanh(ROOT * (p + CUBE * (p * p * p)))
                    h = (p * (0.5 * (1.0 + th))).astype(BF16)
                    hidt[cols(n, hw), cols(r, hr)] = h.T

                hw = 256 if ff % 256 == 0 else 128
                loop(ff // hw, part)

            loop(total // hr, hidden)
            put_dy.wait()
            put_x.wait()

        pl.run_scoped(
            start, pltpu.VMEM((2, rows, d), BF16), pltpu.VMEM((2, 256 if total % 256 == 0 else 128, ff), BF16)
        )
        w_load.wait()

        o1 = jnp.where(z == 0, 1, z - 1)
        o2 = jnp.where(z == END, 1, jnp.where(z == 2, 3, 2))
        o3 = jnp.where(z < 2, 3, 0)

        def pass_z(row, zb, q):
            @pl.when((zb < z) & (z < END))
            def _():
                zcopy(row, zb, q, 1).start()

            @pl.when((zb > z) & (z > 0))
            def _():
                zcopy(row, zb, q, -1).start()

        def chip(i):
            row = jnp.where((i == 0) | (i == 1) | (i == 3) | (i == 6), y, other_y)
            near = jnp.where((i == 0) | (i == 2), z, o1)
            return row, jnp.where(i > 5, o3, jnp.where((i == 3) | (i == 5), o2, near))

        def unpack(code):
            return code // 256, code // 16 % 16, code // 4 % 4, code % 4

        def relay(code):
            i, q, _, _ = unpack(code)
            row, zb = chip(i)

            @pl.when((i > 0) & (row == y))
            def _():
                zcopy(y, zb, q, 1).wait_recv()
                pass_z(y, zb, q)

                @pl.when(q > 0)
                def _():
                    ycopy(y, zb, q).start()

            @pl.when((row != y) & (q == 0) & (i == 2))
            def _():
                ycopy(other_y, z, 0).wait_recv()

                @pl.when(jnp.logical_not(last))
                def _():
                    zcopy(other_y, z, 0, 1).start()

                @pl.when(jnp.logical_not(first))
                def _():
                    zcopy(other_y, z, 0, -1).start()

                @pl.when(first)
                def _():
                    xcopy(0, p_zp, yz).start()

                @pl.when(last)
                def _():
                    xcopy(1, p_zm, yz).start()

            @pl.when((row != y) & (q == 0) & (i != 2))
            def _():
                zcopy(other_y, zb, 0, 1).wait_recv()
                pass_z(other_y, zb, 0)

                @pl.when((i == 4) & (z == 1))
                def _():
                    xcopy(0, p_zp, yz).start()

                @pl.when((i == 5) & (z == 2))
                def _():
                    xcopy(1, p_zm, yz).start()

            @pl.when((row != y) & (q > 0))
            def _():
                @pl.when((i == 7) & (q == nch - 3 + (nch < 4)))
                def _():
                    @pl.when(inner)
                    def _():
                        xcopy(0, p_zp, yz - 1).wait_recv()
                        xcopy(1, p_zm, yz + 1).wait_recv()

                    for v in range(WINDOW):
                        move_x(v)
                        step_out()

                ycopy(other_y, zb, q).wait_recv()

            @pl.when(i > 0)
            def _():
                dcopy(row * NZ + zb, c, q).start()

            @pl.when((i == 7) & (q == nch - 1))
            def _():
                for v in range(WINDOW, LEAD - 1):
                    step_in()
                    move_x(v)
                    step_out()

        def stream(dyc, preu, acc, wte, e_d, e_own, e_out):
            orders = [[relays(inner_chip, nch)[e] for e in range(NY * NZ * nch)] for inner_chip in (False, True)]
            places = len(orders[0])
            ready = 1 + max(e for e, code in enumerate(orders[0]) if code // 256 in (1, 4))

            def at(e):
                code = jnp.where(inner, orders[1][0], orders[0][0])
                for k in range(1, places):
                    code = jnp.where(e == k, jnp.where(inner, orders[1][k], orders[0][k]), code)
                return code

            def get(code, slot):
                i, q, _, _ = unpack(code)
                row, zb = chip(i)
                return pltpu.make_async_copy(
                    fdy_ref.at[row * NZ + zb, :, :, cols(q, ck)], dyc.at[slot], ls1.at[slot]
                )

            def fetch(code, slot):
                i, q, _, _ = unpack(code)
                row, zb = chip(i)
                dcopy(row * NZ + zb, other_c, q).wait_recv()
                get(code, slot).start()

            def get_pre(u, keep):
                at = pl.ds(pl.multiple_of(u * (NC * rows), NC * rows), NC * rows)
                return pltpu.make_async_copy(pre_ref.at[at], preu.at[keep], ls2.at[keep])

            def place(e, codes):
                code, following = codes
                later = at(e + 2)

                @pl.when(e + 2 < places)
                def _():
                    relay(later)

                @pl.when(e + 1 < places)
                def _():
                    fetch(following, (e + 1) % 2)

                i, q, mark, keep = unpack(code)
                row, zb = chip(i)
                u = row * NZ + zb

                @pl.when(mark % 2 == 1)
                def _():
                    get_pre(u, keep).start()

                get(code, e % 2).wait()
                lhs = dyc[e % 2].reshape(NC * rows, ck)
                for n in range(0, ff, fn):
                    term = lax.dot_general(
                        lhs, wdn[n : n + fn, cols(q, ck)], ROW_BY_ROW, preferred_element_type=F32
                    )
                    acc[keep, :, n : n + fn] = jnp.where(mark % 2 == 1, 0.0, acc[keep, :, n : n + fn]) + term

                @pl.when(mark >= 2)
                def _():
                    get_pre(u, keep).wait()

                    def part(n):
                        p = preu[keep, :, cols(n, fn)].astype(F32)
                        pp = p * p
                        th = jnp.tanh(ROOT * (p + CUBE * (p * pp)))
                        slope = 0.5 * (1.0 + th) + (0.5 * p) * (1.0 - th * th) * (ROOT * (1.0 + 3.0 * CUBE * pp))
                        dpre[u, :, :, cols(n, fn)] = (acc[keep, :, cols(n, fn)] * slope).astype(BF16).reshape(NC, rows, fn)

                    loop(ff // fn, part)

                @pl.when(edge)
                def _():
                    early_step(e - ready, wte, e_d, e_own, e_out)

                return following, later

            codes = at(0), at(1)
            relay(codes[0])
            relay(codes[1])
            fetch(codes[0], 0)
            lax.fori_loop(0, places, place, codes)

            @pl.when(edge)
            def _():
                for r in range(nearly - 2, nearly):
                    edcopy(e_d, r).wait_send()
                    ezcopy(r, e_out).wait_send()

        pl.run_scoped(
            stream,
            pltpu.VMEM((2, NC, rows, ck), BF16),
            pltpu.VMEM((3, NC * rows, ff), BF16),
            pltpu.VMEM((3, NC * rows, ff), F32),
            pltpu.VMEM((tn, ff), BF16),
            pltpu.VMEM((2, NY, rows, tn), BF16),
            pltpu.VMEM((2, NY, rows, tn), F32),
            pltpu.VMEM((2, NY, rows, tn), BF16),
        )

    pl.run_scoped(phase1, pltpu.VMEM((ff, d), BF16))

    def all_sent():
        def sent(q):
            def block(zb):
                @pl.when((zb <= z) & (z < END))
                def _():
                    zcopy(y, zb, q, 1).wait_send()

                @pl.when((zb >= z) & (z > 0))
                def _():
                    zcopy(y, zb, q, -1).wait_send()

                @pl.when(q == 0)
                def _():
                    @pl.when((zb <= z) & (z < END))
                    def _():
                        zcopy(other_y, zb, q, 1).wait_send()

                    @pl.when((zb >= z) & (z > 0))
                    def _():
                        zcopy(other_y, zb, q, -1).wait_send()

                @pl.when((q > 0) | (zb == z))
                def _():
                    ycopy(y, zb, q).wait_send()

            loop(NZ, block)
            loop(NY * NZ, lambda b: dcopy(b, c, q).wait_send())

        loop(nch, sent)

        @pl.when(z < 2)
        def _():
            xcopy(0, p_zp, yz).wait_send()

        @pl.when(z >= 2)
        def _():
            xcopy(1, p_zm, yz).wait_send()

    def phase2(own, out_r, out_l, out_d, out_y, ein, wt, dyt, xt, odn, oin, odx, ls):
        steps = nt + TAIL

        def rcopy(slot, k):
            return remote(out_r.at[slot, k], in_r.at[slot, k], s_r.at[slot, k], r_r.at[slot, k], p_zp)

        def lcopy(slot, k):
            return remote(out_l.at[slot, k], in_l.at[slot, k], s_l.at[slot, k], r_l.at[slot, k], p_zm)

        def dsum(slot):
            return remote(out_d.at[slot], in_d.at[slot], s_d.at[slot], r_d.at[slot], p_d)

        def ysum(slot):
            return remote(out_y.at[slot], in_y.at[slot], s_y.at[slot], r_y.at[slot], p_y)

        def add_core(s):
            j = s - 1

            @pl.when(inside(j))
            def _():
                slot, ring = j % DRING, j % OWN
                dsum(slot).wait_recv()

                def piece(b):
                    own[ring, b // NZ, b % NZ] += in_d[slot, b].astype(F32)

                loop(NY * NZ, piece)

        def along(s, away, start, copy, inb, outb):
            behind = z if away == 1 else END - z
            j = s - 1 - behind

            @pl.when(inside(j))
            def _():
                slot, ring = j % RING, j % OWN
                sent = j % 2 == 0
                for k in range(END, 0, -1):
                    zz = z + away * k
                    here = (zz >= 0) & (zz < NZ)
                    if k == 1:
                        here = here & jnp.logical_not(start & sent)

                    @pl.when(here)
                    def _():
                        @pl.when(j >= RING)
                        def _():
                            copy(slot, k - 1).wait_send()

                        @pl.when(start)
                        def _():
                            def piece(h):
                                outb[slot, k - 1, h] = own[ring, h, zz].astype(BF16)

                            loop(NY, piece)

                        if k < END:

                            @pl.when(jnp.logical_not(start))
                            def _():
                                copy(slot, k).wait_recv()

                                def piece(h):
                                    outb[slot, k - 1, h] = (own[ring, h, zz] + inb[slot, k, h].astype(F32)).astype(BF16)

                                loop(NY, piece)

                        copy(slot, k - 1).start()

        def settle(s, away, copy, inb):
            behind = z if away == 1 else END - z
            j = s - behind - jnp.where(behind == END, 1, 2)

            @pl.when(inside(j) & ((behind > 1) | ((behind == 1) & (j % 2 == 1))))
            def _():
                slot, ring = j % RING, j % OWN
                copy(slot, 0).wait_recv()

                def piece(h):
                    own[ring, h, z] += inb[slot, 0, h].astype(F32)

                loop(NY, piece)

        def get_early(r):
            return pltpu.make_async_copy(fe_ref.at[r], ein.at[r % 2], ls.at[6, r % 2])

        def take_early(s):
            @pl.when(inner & (s % 2 == 0) & inside(s - 4))
            def _():
                r, ring = (s - 4) // 2, (s - 4) % OWN
                get_early(r).wait()
                own[ring, :, z] += ein[r % 2].astype(F32)

            @pl.when(inner & (s % 2 == 0) & inside(s - 2))
            def _():
                r = (s - 2) // 2
                ezcopy(r).wait_recv()
                get_early(r).start()

        def across(s):
            j = s - 4

            @pl.when(inside(j))
            def _():
                slot, ring = j % RING, j % OWN

                @pl.when(j >= RING)
                def _():
                    ysum(slot).wait_send()

                out_y[slot] = own[ring, other_y, z].astype(BF16)
                ysum(slot).start()

        def put_dx(j):
            return pltpu.make_async_copy(odx.at[j % 2], dx_ref.at[:, cols(j, tn)], ls.at[5, j % 2])

        def finish(s):
            j = s - 6

            @pl.when(inside(j))
            def _():
                slot, ring = j % RING, j % OWN

                @pl.when(j >= 2)
                def _():
                    put_dx(j - 2).wait()

                ysum(slot).wait_recv()
                odx[j % 2] = (own[ring, y, z] + in_y[slot].astype(F32)).astype(BF16)
                put_dx(j).start()

        def get_x(j):
            return pltpu.make_async_copy(fx_ref.at[:, :, :, cols(j, tn)], xt.at[j % 2], ls.at[2, j % 2])

        def get_w(j):
            return pltpu.make_async_copy(win_ref.at[cols(j, tn)], wt.at[j % 2], ls.at[0, j % 2])

        def get_dy(j):
            return pltpu.make_async_copy(fdy_ref.at[:, :, :, cols(j, tn)], dyt.at[j % 2], ls.at[1, j % 2])

        def put_dn(j):
            return pltpu.make_async_copy(odn.at[j % 2], dwdn_ref.at[:, cols(j, tn)], ls.at[3, j % 2])

        def put_in(j):
            return pltpu.make_async_copy(oin.at[j % 2], dwin_ref.at[cols(j, tn)], ls.at[4, j % 2])

        def term(j):
            slot, ring = j % DRING, j % OWN
            get_w(j).wait()

            @pl.when(j + 1 < nt)
            def _():
                get_w(j + 1).start()

            @pl.when(j >= DRING)
            def _():
                dsum(slot).wait_send()

            def dot(core, h):
                lhs = dpre[h * NZ : (h + 1) * NZ, core].reshape(NZ * rows, ff)
                return lax.dot_general(
                    lhs, wt[j % 2], ROW_BY_ROW, preferred_element_type=F32
                ).reshape(NZ, rows, tn)

            for h in range(NY):
                out_d[slot, h * NZ : (h + 1) * NZ] = dot(other_c, h).astype(BF16)
            dsum(slot).start()
            for h in range(NY):
                own[ring, h] = dot(c, h)

        def down(j):
            get_dy(j).wait()

            @pl.when(j + 1 < nt)
            def _():
                get_dy(j + 1).start()

            @pl.when(j >= 2)
            def _():
                put_dn(j - 2).wait()

            rhs = dyt[j % 2].reshape(total, tn)
            for m in range(0, ff, ff // 4):
                odn[j % 2, m : m + ff // 4] = jnp.dot(
                    hidt[m : m + ff // 4], rhs, preferred_element_type=F32
                ).astype(BF16)
            put_dn(j).start()

        def inward(j):
            get_x(j).wait()

            @pl.when(j >= 2)
            def _():
                put_in(j - 2).wait()

            lhs = xt[j % 2].reshape(total, tn)
            for n in range(0, ff, ff // 2):
                oin[j % 2, :, n : n + ff // 2] = lax.dot_general(
                    lhs, dpre[:, :, :, n : n + ff // 2].reshape(total, ff // 2), (((0,), (0,)), ((), ())),
                    preferred_element_type=F32,
                ).astype(BF16)
            put_in(j).start()

        get_w(0).start()
        get_dy(0).start()

        step_in()
        move_x(LEAD - 1)
        step_out()

        def step(s):
            step_in()
            add_core(s)
            along(s, 1, first, rcopy, in_r, out_r)
            along(s, -1, last, lcopy, in_l, out_l)
            settle(s, 1, rcopy, in_r)
            settle(s, -1, lcopy, in_l)
            take_early(s)
            across(s)
            finish(s)
            move_x(s + LEAD)

            @pl.when(s < steps - WINDOW)
            def _():
                step_out()

            @pl.when(s < nt)
            def _():
                term(s)

            @pl.when(s == nt + 1)
            def _():
                all_sent()

            @pl.when(inside(s - 1))
            def _():
                xd(s - 1, other_c).wait_recv()
                get_x(s - 1).start()

            m = s - s // 9 - 1

            @pl.when((s % 9 != 0) & (m < nt))
            def _():
                down(m)

            @pl.when(inside(s - 1))
            def _():
                inward(s - 1)

        loop(steps, step)
        loop(2, lambda i: finish(steps + i))

        for j in range(nt - RING, nt):
            slot = j % RING
            for k in range(END):
                early = k == 0 and j % 2 == 0

                @pl.when((z + k + 1 < NZ) & jnp.logical_not(first & early))
                def _():
                    rcopy(slot, k).wait_send()

                @pl.when((z - k - 1 >= 0) & jnp.logical_not(last & early))
                def _():
                    lcopy(slot, k).wait_send()

            ysum(slot).wait_send()
            xy(j, y).wait_send()
            xd(j, c).wait_send()
            x_out(j, 1, True)
            x_out(j, -1, True)

            @pl.when(z == 2)
            def _():
                xz(j, 1, 1, 0).wait_send()

            @pl.when(z == 1)
            def _():
                xz(j, -1, 1, END).wait_send()

        for j in range(nt - DRING, nt):
            dsum(j % DRING).wait_send()

        for j in range(nt - 2, nt):
            put_dn(j).wait()
            put_in(j).wait()
            put_dx(j).wait()

    pl.run_scoped(
        phase2,
        pltpu.VMEM((OWN, NY, NZ, rows, tn), F32),
        pltpu.VMEM((RING, END, NY, rows, tn), BF16),
        pltpu.VMEM((RING, END, NY, rows, tn), BF16),
        pltpu.VMEM((DRING, NY * NZ, rows, tn), BF16),
        pltpu.VMEM((RING, rows, tn), BF16),
        pltpu.VMEM((2, NY, rows, tn), BF16),
        pltpu.VMEM((2, tn, ff), BF16),
        pltpu.VMEM((2, NY * NZ, NC, rows, tn), BF16),
        pltpu.VMEM((2, NY * NZ, NC, rows, tn), BF16),
        pltpu.VMEM((2, ff, tn), BF16),
        pltpu.VMEM((2, tn, ff), BF16),
        pltpu.VMEM((2, rows, tn), BF16),
        pltpu.SemaphoreType.DMA((7, 2)),
    )


def call(rows, d, ff, tn, nch, fn, x, dy, pre, win, wdn):
    blocks = NY * NZ
    total = blocks * NC * rows
    dma = pltpu.SemaphoreType.DMA
    early = (d // tn + 1) // 2
    any_ = pl.BlockSpec(memory_space=pl.ANY)
    return pl.pallas_call(
        functools.partial(bwd_kernel, (rows, d, ff, tn, nch, fn)),
        name="bwd",
        out_shape=[
            jax.ShapeDtypeStruct((rows, d), BF16),
            jax.ShapeDtypeStruct((d, ff), BF16),
            jax.ShapeDtypeStruct((ff, d), BF16),
            jax.ShapeDtypeStruct((blocks, NC, rows, d), BF16),
            jax.ShapeDtypeStruct((blocks, NC, rows, d), BF16),
            jax.ShapeDtypeStruct((early, NY, rows, tn), BF16),
        ],
        in_specs=[any_] * 5,
        out_specs=[any_] * 6,
        scratch_shapes=[
            pltpu.VMEM((blocks, NC, rows, ff), BF16),
            pltpu.VMEM((ff, total), BF16),
            pltpu.VMEM((RING, END, NY, rows, tn), BF16),
            pltpu.VMEM((RING, END, NY, rows, tn), BF16),
            pltpu.VMEM((DRING, blocks, rows, tn), BF16),
            pltpu.VMEM((RING, rows, tn), BF16),
            dma((NZ, nch + 1)), dma((NZ, nch)), dma((blocks, nch)),
            dma((NZ, nch + 1)), dma((NZ, nch + 1)), dma((NZ, nch)), dma((blocks, nch)),
            dma((2,)), dma((2,)), dma((3,)), dma((2,)), dma((3,)), dma((1,)),
            dma((RING, END)), dma((RING, END)), dma((DRING,)), dma((RING,)), dma((DRING,)), dma((early,)),
            dma((RING, END)), dma((RING, END)), dma((DRING,)), dma((RING,)), dma((2,)), dma((2,)),
            dma((2, 2, RING)), dma((2, 2, RING)), dma((RING,)), dma((RING,)), dma((RING,)), dma((RING,)),
            pltpu.SemaphoreType.REGULAR((4,)),
        ],
        compiler_params=pltpu.CompilerParams(
            collective_id=0, has_side_effects=True, vmem_limit_bytes=67043328
        ),
    )(x, dy, pre, win, wdn)


def solution(mesh):
    spec = jax.sharding.PartitionSpec
    rows_of, cols_of = spec(("dp", "tp"), None), spec("dp", "tp")

    def local(x, dy, pre, win, wdn):
        rows, d = x.shape
        ff = pre.shape[1]
        dx, dwin, dwdn = call(rows, d, ff, 256, 7, 256, x, dy, pre, win, wdn)[:3]
        return dx, dwin, dwdn

    return jax.shard_map(
        local,
        mesh=mesh,
        in_specs=(rows_of, rows_of, cols_of, spec(None, "tp"), spec("tp", None)),
        out_specs=(rows_of, cols_of, rows_of),
        check_vma=False,
    )
```
